32 devices in a mesh: section: 2 (over core), seq: 16 (over z, y, x).
Axes of the slice: x: 2, y: 2, z: 4, core: 2. Of those that a mesh axis runs over, the one named last changes fastest.
Arguments:
- acts: bfloat16 [2, 4096, 2048], P('section', 'seq'), may hold values from -6 to 6
- in_proj: bfloat16 [2, 2048, 4640], P('section', 'seq'), may hold values from -0.125 to 0.125
- out_proj: bfloat16 [2, 2048, 2048], P('section'), may hold values from -0.125 to 0.125
- conv_weight: float32 [2, 4, 2304], P('section'), may hold values from -3 to 3
- conv_bias: float32 [2, 2304], P('section'), may hold values from -3 to 3
- dt_bias: float32 [2, 32], P('section'), may hold values from -4 to -1
- decay_rate: float32 [2, 32], P('section'), may hold values from 0.0001 to 0.5
- skip_gain: float32 [2, 32], P('section'), may hold values from -4 to 4
- level_bias: float32 [2, 256], P('section'), may hold values from -4 to 4
- norm_gain: float32 [2, 2048], P('section'), may hold values from 0.5 to 1.5
- gate_gain: float32 [2, 2048], P('section'), may hold values from 0.5 to 1.5
Outputs:
- handoff: bfloat16 [2, 4096, 2048], P('section', 'seq')
The draws below stay inside these ranges and needn't reach their ends.
All inputs are finite; a program needn't handle non-finite values.
Results may differ from the reference program's by a relative error of at most 0.006.
Values may be sent and summed in bfloat16 or wider, within the bound.
A program may use at most 128 MiB of HBM per device.

```python
import math
import jax
import jax.numpy as jnp
from jax import lax

D = 2048
CONV = 4
HEADS = 32
LEVELS = 8
SECTIONS = 2
DI = 2048
CH = 2304
PROJ = 4640
SEQLEN = 4096
N_SEQ = 16


def block_levels(key, extent, shards, low, largest):
    loudness = 1.0
    for axis_at, parts in shards:
        steps = jax.random.uniform(jax.random.fold_in(jax.random.fold_in(key, 6), axis_at), (parts,), jnp.float32, low / len(shards), largest / len(shards))
        loudness = loudness * jnp.repeat(jnp.exp(steps), extent[axis_at] // parts).reshape((-1,) + (1,) * (len(extent) - 1 - axis_at))
    return loudness


def normal_values(key, extent, width, reach, pieces=(), kind=jnp.bfloat16):
    loudness = block_levels(key, extent, pieces, -0.22, 0.18) if pieces else 1.0
    values = jax.random.normal(key, extent, jnp.float32) * width * loudness
    return jnp.minimum(jnp.maximum(values, -reach), reach).astype(kind)


def setup_inputs(seed: int = 0) -> dict:
    streams_of = jax.random.split(jax.random.key(seed), 12)
    acts = normal_values(streams_of[0], (SECTIONS, SEQLEN, D), 1.0, 6.0, ((0, 2), (1, 16)))
    in_proj = normal_values(streams_of[1], (SECTIONS, D, PROJ), D ** -0.5, 0.125, ((0, 2), (1, 16)))
    out_proj = normal_values(streams_of[2], (SECTIONS, DI, D), DI ** -0.5, 0.125, ((0, 2),))
    conv_weight = normal_values(streams_of[3], (SECTIONS, CONV, CH), 0.6, 3.0, ((0, 2),), jnp.float32)
    conv_bias = normal_values(streams_of[4], (SECTIONS, CH), 0.5, 3.0, ((0, 2),), jnp.float32)
    dt_bias = jnp.clip(-4.0 + 3.0 * jax.random.uniform(streams_of[5], (SECTIONS, HEADS), jnp.float32) ** block_levels(streams_of[5], (SECTIONS, HEADS), ((0, 2),), -0.2, 0.2), -4.0, -1.0)
    decay_rate = jnp.clip(jnp.exp(math.log(0.5) - 8.517193 * jax.random.uniform(streams_of[6], (SECTIONS, HEADS), jnp.float32) ** block_levels(streams_of[6], (SECTIONS, HEADS), ((0, 2),), -0.2, 0.2)), 0.0001, 0.5)
    skip_gain = normal_values(streams_of[7], (SECTIONS, HEADS), 1.0, 4.0, ((0, 2),), jnp.float32)
    level_bias = normal_values(streams_of[8], (SECTIONS, HEADS * LEVELS), 1.0, 4.0, ((0, 2),), jnp.float32)
    norm_gain = jnp.clip(1.0 + 0.1 * jax.random.normal(streams_of[9], (SECTIONS, D), jnp.float32), 0.5, 1.5)
    gate_gain = jnp.clip(1.0 + 0.1 * jax.random.normal(streams_of[10], (SECTIONS, DI), jnp.float32), 0.5, 1.5)
    return dict(acts=acts, in_proj=in_proj, out_proj=out_proj, conv_weight=conv_weight, conv_bias=conv_bias, dt_bias=dt_bias, decay_rate=decay_rate, skip_gain=skip_gain, level_bias=level_bias, norm_gain=norm_gain, gate_gain=gate_gain)


EPS = 1e-05
best_precision = lax.Precision.HIGHEST

def block_core(operands):
    c_block, b_block, x_block, cum_block, dt_block, lam_block = operands
    length = c_block.shape[0]
    scores = jnp.dot(c_block, b_block.T, precision=best_precision, preferred_element_type=jnp.float32)
    row_ids = lax.broadcasted_iota(jnp.int32, (length, length), 0)
    col_ids = lax.broadcasted_iota(jnp.int32, (length, length), 1)
    causal = (col_ids <= row_ids)[:, :, None]
    differ = cum_block[:, None, :] - cum_block[None, :, :]
    decays = jnp.where(causal, jnp.exp(jnp.where(causal, differ, 0.0)), 0.0)
    weights = decays * scores[:, :, None] * dt_block[None, :, :] * lam_block[:, None, :]
    y_block = jnp.einsum('tsh,shp->thp', weights, x_block, precision=best_precision)
    tail = jnp.exp(cum_block[-1][None, :] - cum_block) * dt_block
    state = jnp.einsum('sn,shp->hnp', b_block, x_block * tail[:, :, None], precision=best_precision)
    return (y_block, state)

def mixer(acts, w_in, w_out, conv_w, conv_b, dt_b, rate, skip, lam_b, gain_in, gain_gate):
    hidden = acts.astype(jnp.float32)
    seqlen = hidden.shape[0]
    inner = gain_gate.shape[0]
    heads = dt_b.shape[0]
    head_size = inner // heads
    chans = conv_w.shape[1]
    state_size = (chans - inner) // 2
    kernel_len = conv_w.shape[0]
    normed_in = (hidden * lax.rsqrt(lax.optimization_barrier(jnp.mean(hidden * hidden, axis=1, keepdims=True)) + EPS) * gain_in).astype(jnp.bfloat16)
    projected = jnp.dot(normed_in, w_in, preferred_element_type=jnp.float32).astype(jnp.bfloat16)
    conv_in = jnp.concatenate([jnp.zeros((kernel_len - 1, chans), jnp.float32), projected[:, :chans].astype(jnp.float32)], axis=0)
    mixed = conv_b + jnp.zeros((seqlen, chans), jnp.float32)
    for offset in range(kernel_len):
        mixed = mixed + conv_w[offset] * conv_in[offset:offset + seqlen]
    mixed = jax.nn.silu(mixed)
    values = mixed[:, :inner].reshape(seqlen, heads, head_size)
    b_mat = mixed[:, inner:inner + state_size]
    c_mat = mixed[:, inner + state_size:]
    z_gate = projected[:, chans:chans + inner].astype(jnp.float32)
    steps = jax.nn.softplus(projected[:, chans + inner:chans + inner + heads].astype(jnp.float32) + dt_b)
    lam = jax.nn.softplus(projected[:, chans + inner + heads:].astype(jnp.float32) + lam_b).reshape(seqlen, heads, LEVELS)
    blocks = N_SEQ
    length = seqlen // blocks
    log_decay = (-steps * rate).reshape(blocks, length, heads)
    cum = jnp.cumsum(log_decay, axis=1)
    x_blocks = values.reshape(blocks, length, heads, head_size)
    b_blocks = b_mat.reshape(blocks, length, state_size)
    c_blocks = c_mat.reshape(blocks, length, state_size)
    dt_blocks = steps.reshape(blocks, length, heads)
    lam_blocks = lam.reshape(blocks, length, heads, LEVELS)
    y_all, states = lax.map(block_core, (c_blocks, b_blocks, x_blocks, cum, dt_blocks, lam_blocks[..., 0]))
    y_all = y_all + skip[None, None, :, None] * x_blocks
    endlog = cum[:, -1, :]
    inclusive = jnp.cumsum(endlog, axis=0)
    exclusive = inclusive - endlog
    for level in range(1, blocks.bit_length()):
        half = 2 ** (level - 1)
        groups = blocks // (2 * half)
        lower_states = states.reshape(groups, 2, half, heads, state_size, head_size)[:, 0]
        incl_groups = inclusive.reshape(groups, 2, half, heads)
        lower_end = incl_groups[:, 0, half - 1]
        weights = jnp.exp(lower_end[:, None, :] - incl_groups[:, 0])
        summed = jnp.einsum('gjh,gjhnp->ghnp', weights, lower_states, precision=best_precision)
        upper_excl = exclusive.reshape(groups, 2, half, heads)[:, 1]
        carry = jnp.exp(upper_excl - lower_end[:, None, :])
        c_upper = c_blocks.reshape(groups, 2, half, length, state_size)[:, 1]
        reads = jnp.einsum('gitn,ghnp->githp', c_upper, summed, precision=best_precision)
        cum_upper = cum.reshape(groups, 2, half, length, heads)[:, 1]
        lam_upper = lam_blocks.reshape(groups, 2, half, length, heads, LEVELS)[:, 1, :, :, :, level]
        scale = carry[:, :, None, :] * jnp.exp(cum_upper) * lam_upper
        shaped = y_all.reshape(groups, 2, half, length, heads, head_size)
        y_all = shaped.at[:, 1].add(reads * scale[..., None]).reshape(blocks, length, heads, head_size)
    y_flat = y_all.reshape(seqlen, inner)
    gated = y_flat * jax.nn.silu(z_gate)
    normed = (gated * lax.rsqrt(lax.optimization_barrier(jnp.mean(gated * gated, axis=1, keepdims=True)) + EPS) * gain_gate).astype(jnp.bfloat16)
    return (hidden + jnp.dot(normed, w_out, preferred_element_type=jnp.float32)).astype(jnp.bfloat16)

def reference(acts, in_proj, out_proj, conv_weight, conv_bias, dt_bias, decay_rate, skip_gain, level_bias, norm_gain, gate_gain):
    results = []
    for section_id in range(SECTIONS):
        results.append(mixer(acts[section_id], in_proj[section_id], out_proj[section_id], conv_weight[section_id], conv_bias[section_id], dt_bias[section_id], decay_rate[section_id], skip_gain[section_id], level_bias[section_id], norm_gain[section_id], gate_gain[section_id]))
    stacked = jnp.stack(results, axis=0)
    return jnp.roll(stacked, 1, axis=0)
```

```python
import functools

import jax
import jax.numpy as jnp
from jax import lax
from jax.experimental import pallas as pl
from jax.experimental.pallas import tpu as pltpu
from jax.sharding import PartitionSpec as P

EPS = 1e-05
MESH = pl.DeviceIdType.MESH
f32 = jnp.float32
bf16 = jnp.bfloat16


def remote(src, dst, send, recv, seq):
    return pltpu.make_async_remote_copy(
        src_ref=src,
        dst_ref=dst,
        send_sem=send,
        recv_sem=recv,
        device_id={"seq": seq},
        device_id_type=MESH,
    )


def greet(seq):
    pl.semaphore_signal(
        pltpu.get_barrier_semaphore(), inc=1, device_id={"seq": seq}, device_id_type=MESH
    )


def gather_kernel(
    group, n, u_ref, w_ref, u_all, w_all, u_send, u_recv, w_send, up_send, down_send, w_recv, own_sem
):
    me = lax.axis_index("seq")
    outer = me // group
    inner = lax.rem(me, group)
    outers = n // group
    base = outer * group
    has_up = outer < outers - 1
    has_down = outer > 0
    barrier = pltpu.get_barrier_semaphore()
    for step in range(1, group):
        greet(base + lax.rem(inner + step, group))

    @pl.when(has_up)
    def _():
        greet(me + group)

    @pl.when(has_down)
    def _():
        greet(me - group)

    pl.semaphore_wait(
        barrier, group - 1 + has_up.astype(jnp.int32) + has_down.astype(jnp.int32)
    )

    own_w = pltpu.make_async_copy(w_ref.at[inner], w_all.at[me], own_sem.at[0])
    own_w.start()
    own_u = pltpu.make_async_copy(u_ref, u_all.at[inner], own_sem.at[1])
    own_u.start()

    def up(src, piece):
        return remote(src, w_all.at[piece], up_send.at[piece], w_recv.at[piece], me + group)

    def down(src, piece):
        return remote(src, w_all.at[piece], down_send.at[piece], w_recv.at[piece], me - group)

    def arrived(piece):
        remote(w_all.at[piece], w_all.at[piece], w_send.at[0], w_recv.at[piece], me).wait_recv()

    sends = []
    for step in range(1, group):
        peer = lax.rem(inner + step, group)
        copy = remote(w_ref.at[peer], w_all.at[me], w_send.at[step], w_recv.at[me], base + peer)
        copy.start()
        sends.append(copy)

    @pl.when(has_up)
    def _():
        up(w_ref.at[inner], me).start()

    @pl.when(has_down)
    def _():
        down(w_ref.at[inner], me).start()

    for step in range(1, group):
        peer = lax.rem(inner + step, group)
        copy = remote(u_ref, u_all.at[inner], u_send.at[step], u_recv.at[inner], base + peer)
        copy.start()
        sends.append(copy)

    for step in range(1, group):
        piece = base + lax.rem(inner + step, group)
        arrived(piece)

        @pl.when(has_up)
        def _():
            up(w_all.at[piece], piece).start()

        @pl.when(has_down)
        def _():
            down(w_all.at[piece], piece).start()

    def relay(distance, carry):
        for step in range(group):
            slot = lax.rem(inner + step, group)

            @pl.when(outer - distance >= 0)
            def _():
                piece = (outer - distance) * group + slot
                arrived(piece)

                @pl.when(has_up)
                def _():
                    up(w_all.at[piece], piece).start()

            @pl.when(outer + distance < outers)
            def _():
                piece = (outer + distance) * group + slot
                arrived(piece)

                @pl.when(has_down)
                def _():
                    down(w_all.at[piece], piece).start()

        return carry

    lax.fori_loop(1, outers, relay, 0)

    def drain(piece, carry):
        source = piece // group

        @pl.when(jnp.logical_and(has_up, source <= outer))
        def _():
            up(w_all.at[piece], piece).wait_send()

        @pl.when(jnp.logical_and(has_down, source >= outer))
        def _():
            down(w_all.at[piece], piece).wait_send()

        return carry

    lax.fori_loop(0, n, drain, 0)
    for copy in sends:
        copy.wait_send()
    for step in range(1, group):
        peer = lax.rem(inner + step, group)
        remote(u_ref, u_all.at[peer], u_send.at[0], u_recv.at[peer], me).wait_recv()
    own_w.wait()
    own_u.wait()


def gathered(u, w_parts, n):
    group = w_parts.shape[0]
    dma = pltpu.SemaphoreType.DMA
    return pl.pallas_call(
        functools.partial(gather_kernel, group, n),
        out_shape=(
            jax.ShapeDtypeStruct((group,) + u.shape, u.dtype),
            jax.ShapeDtypeStruct((n,) + w_parts.shape[1:], w_parts.dtype),
        ),
        in_specs=[pl.BlockSpec(memory_space=pltpu.VMEM)] * 2,
        out_specs=[pl.BlockSpec(memory_space=pl.ANY)] * 2,
        scratch_shapes=[
            dma((group,)),
            dma((group,)),
            dma((group,)),
            dma((n,)),
            dma((n,)),
            dma((n,)),
            dma((2,)),
        ],
        compiler_params=pltpu.CompilerParams(collective_id=0, has_side_effects=True),
    )(u, w_parts)


def exchange_kernel(group, x_ref, out_ref, send_sem, recv_sem, own_sem):
    me = lax.axis_index("seq")
    inner = lax.rem(me, group)
    base = me - inner
    for step in range(1, group):
        greet(base + lax.rem(inner + step, group))
    pl.semaphore_wait(pltpu.get_barrier_semaphore(), group - 1)
    sends = []
    for step in range(1, group):
        peer = lax.rem(inner + step, group)
        copy = remote(
            x_ref.at[peer], out_ref.at[inner], send_sem.at[step], recv_sem.at[inner], base + peer
        )
        copy.start()
        sends.append(copy)
    own = pltpu.make_async_copy(x_ref.at[inner], out_ref.at[inner], own_sem)
    own.start()
    own.wait()
    for step in range(1, group):
        peer = lax.rem(inner + step, group)
        remote(x_ref.at[peer], out_ref.at[peer], send_sem.at[0], recv_sem.at[peer], me).wait_recv()
    for copy in sends:
        copy.wait_send()


def exchanged(x):
    group = x.shape[0]
    dma = pltpu.SemaphoreType.DMA
    return pl.pallas_call(
        functools.partial(exchange_kernel, group),
        out_shape=jax.ShapeDtypeStruct(x.shape, x.dtype),
        in_specs=[pl.BlockSpec(memory_space=pltpu.VMEM)],
        out_specs=pl.BlockSpec(memory_space=pltpu.VMEM),
        scratch_shapes=[dma((group,)), dma((group,)), dma],
        compiler_params=pltpu.CompilerParams(collective_id=1, has_side_effects=True),
    )(x)


def swapped(block, axis, apart):
    count = lax.axis_size(axis)
    route = []
    for low in range(count):
        high = low | 1 << apart
        if high != low and high < count:
            route += [(low, high), (high, low)]
    return lax.ppermute(block, axis, route)


def from_behind(block, axis, distance):
    devices = range(lax.axis_size(axis))
    route = [(i - distance, i) for i in devices if i - distance in devices]
    return lax.ppermute(block, axis, route)


def passed_along(value, axis, steps):
    count = lax.axis_size(axis)
    pairs = [(source, (source + steps) % count) for source in range(count)]
    return lax.ppermute(value, axis, pairs)


def per_device(
    acts,
    in_proj,
    out_proj,
    conv_weight,
    conv_bias,
    dt_bias,
    decay_rate,
    skip_gain,
    level_bias,
    norm_gain,
    gate_gain,
):
    n = lax.axis_size("seq")
    group = min(4, n)
    bits = group.bit_length() - 1
    position = lax.axis_index("seq")
    inner_at = lax.rem(position, group)
    hidden = acts[0].astype(f32)
    length = hidden.shape[0]
    inner = gate_gain.shape[1]
    heads = dt_bias.shape[1]
    head_size = inner // heads
    chans = conv_weight.shape[2]
    state = (chans - inner) // 2
    taps = conv_weight.shape[1]
    margin = taps - 1
    levels_all = level_bias.shape[1] // heads
    levels_used = n.bit_length() - 1
    wide = inner // group
    hs = heads // group
    tokens = group * length

    w = in_proj[0]
    rows = w.shape[0]

    def cut(lo, count):
        part = w[:, lo : lo + count].reshape(rows, group, count // group)
        return jnp.swapaxes(part, 0, 1)

    shared = jnp.broadcast_to(w[:, inner:chans][None], (group, rows, 2 * state))
    tail = hs + hs * levels_all
    used = 2 * wide + 2 * state + tail
    padded = -(-used // 128) * 128
    w_parts = jnp.concatenate(
        [
            cut(0, inner),
            shared,
            cut(chans, inner),
            cut(chans + inner, heads),
            cut(chans + inner + heads, heads * levels_all),
            jnp.zeros((group, rows, padded - used), w.dtype),
        ],
        axis=2,
    )
    u = (
        hidden * lax.rsqrt(jnp.mean(hidden * hidden, axis=1, keepdims=True) + EPS) * norm_gain[0]
    ).astype(bf16)
    u_all, w_all = gathered(u, w_parts, n)
    p = jnp.dot(
        u_all.reshape(tokens, -1), w_all.reshape(-1, padded), preferred_element_type=f32
    ).astype(bf16)

    def mine(vector, count):
        return lax.dynamic_slice_in_dim(vector, inner_at * count, count, axis=-1)

    mixed_ch = wide + 2 * state
    own_rows = p[:, :mixed_ch]
    earlier = from_behind(own_rows[tokens - margin :], "seq", group)
    taps_w = jnp.concatenate([mine(conv_weight[0][:, :inner], wide), conv_weight[0][:, inner:]], 1)
    taps_b = jnp.concatenate([mine(conv_bias[0][:inner], wide), conv_bias[0][inner:]], 0)
    conv_in = jnp.concatenate([earlier, own_rows], axis=0).astype(f32)
    mixed = taps_b + jnp.zeros((tokens, mixed_ch), f32)
    for offset in range(taps):
        mixed = mixed + taps_w[offset] * conv_in[offset : offset + tokens]
    mixed = jax.nn.silu(mixed)
    values = mixed[:, :wide].reshape(group, length, hs, head_size)
    b_mat = mixed[:, wide : wide + state].reshape(group, length, state).astype(bf16)
    c_mat = mixed[:, wide + state :].reshape(group, length, state).astype(bf16)
    z_gate = p[:, mixed_ch : mixed_ch + wide].astype(f32)
    at = mixed_ch + wide
    steps = jax.nn.softplus(p[:, at : at + hs].astype(f32) + mine(dt_bias[0], hs))
    steps = steps.reshape(group, length, hs)
    lam = jax.nn.softplus(
        p[:, at + hs : at + tail].astype(f32) + mine(level_bias[0], hs * levels_all)
    ).reshape(group, length, hs, levels_all)
    cum = jnp.cumsum(-steps * mine(decay_rate[0], hs), axis=1)
    ends = cum[:, -1]

    scores = jnp.einsum("btn,bsn->bts", c_mat, b_mat, preferred_element_type=f32)
    cum_t = jnp.swapaxes(cum, 1, 2)
    steps_t = jnp.swapaxes(steps, 1, 2)
    lam0_t = jnp.swapaxes(lam[..., 0], 1, 2)
    row_ids = lax.broadcasted_iota(jnp.int32, (length, length), 0)
    col_ids = lax.broadcasted_iota(jnp.int32, (length, length), 1)
    causal = (col_ids <= row_ids)[None, None]
    differ = cum_t[:, :, :, None] - cum_t[:, :, None, :]
    decays = jnp.exp(jnp.where(causal, differ, -jnp.inf))
    weights = decays * scores[:, None] * (steps_t[:, :, None, :] * lam0_t[:, :, :, None])
    x_bf = values.astype(bf16)
    y = jnp.einsum("bhts,bshp->bthp", weights.astype(bf16), x_bf, preferred_element_type=f32)

    tails = jnp.exp(ends[:, None] - cum) * steps
    states = jnp.einsum(
        "bsn,bshp->bhnp", b_mat, (values * tails[..., None]).astype(bf16), preferred_element_type=f32
    )

    def faded(log, block):
        return jnp.exp(log)[..., None, None] * block

    buckets = [[] for _ in range(group)]
    summed = [states[b] for b in range(group)]
    logs = [ends[b] for b in range(group)]
    before = [jnp.zeros_like(ends[0]) for _ in range(group)]
    for bit in range(bits):
        half = 1 << bit
        merged, merged_logs = [], []
        for g in range(len(summed) // 2):
            low, high = summed[2 * g], summed[2 * g + 1]
            for b in range(2 * g * half, 2 * g * half + half):
                buckets[b].append(None)
            for b in range(2 * g * half + half, 2 * (g + 1) * half):
                buckets[b].append(faded(before[b], low))
                before[b] = before[b] + logs[2 * g]
            merged.append(faded(logs[2 * g + 1], low) + high)
            merged_logs.append(logs[2 * g] + logs[2 * g + 1])
        summed, logs = merged, merged_logs
    block_state, block_log = summed[0], logs[0]
    before_log = jnp.zeros_like(block_log)
    for bit in range(bits, levels_used):
        other_log, other_state = swapped((block_log, block_state), "seq", bit)
        upper = position >> bit & 1 == 1
        bucket = jnp.where(upper, faded(before_log, other_state), 0.0)
        for b in range(group):
            buckets[b].append(faded(before[b], bucket))
        merged_upper = faded(block_log, other_state) + block_state
        merged_lower = faded(other_log, block_state) + other_state
        block_state = jnp.where(upper, merged_upper, merged_lower)
        before_log = jnp.where(upper, before_log + other_log, before_log)
        block_log = block_log + other_log

    zero = jnp.zeros_like(states[0])
    stacked = jnp.stack(
        [jnp.stack([zero if s is None else s for s in buckets[b]]) for b in range(group)]
    )
    reads = jnp.einsum(
        "btn,blhnp->btlhp", c_mat, stacked.astype(bf16), preferred_element_type=f32
    )
    scale = lam[..., 1 : levels_used + 1] * jnp.exp(cum)[..., None]
    for level in range(levels_used):
        y = y + scale[..., level][..., None] * reads[:, :, level]
    y = y + mine(skip_gain[0], hs)[:, None] * values
    gated = y.reshape(tokens, wide) * jax.nn.silu(z_gate)

    own = exchanged(gated.astype(bf16).reshape(group, length, wide))
    own = jnp.swapaxes(own, 0, 1).reshape(length, inner).astype(f32)
    normed = (
        own * lax.rsqrt(jnp.mean(own * own, axis=1, keepdims=True) + EPS) * gate_gain[0]
    ).astype(bf16)
    result = (hidden + jnp.dot(normed, out_proj[0], preferred_element_type=f32)).astype(bf16)
    moved = passed_along(result, "section", 1)
    return moved[None]


def solution(mesh):
    return jax.shard_map(
        per_device,
        mesh=mesh,
        in_specs=(
            P("section", "seq", None),
            P("section", "seq", None),
            P("section", None, None),
            P("section", None, None),
            P("section", None),
            P("section", None),
            P("section", None),
            P("section", None),
            P("section", None),
            P("section", None),
            P("section", None),
        ),
        out_specs=P("section", "seq", None),
        check_vma=False,
    )
```

```python
import functools

import jax
import jax.numpy as jnp
from jax import lax
from jax.experimental import pallas as pl
from jax.experimental.pallas import tpu as pltpu
from jax.sharding import PartitionSpec as P

EPS = 1e-05
MESH = pl.DeviceIdType.MESH
f32 = jnp.float32
bf16 = jnp.bfloat16


def remote(src, dst, send, recv, seq):
    return pltpu.make_async_remote_copy(
        src_ref=src,
        dst_ref=dst,
        send_sem=send,
        recv_sem=recv,
        device_id={"seq": seq},
        device_id_type=MESH,
    )


def greet(seq):
    pl.semaphore_signal(
        pltpu.get_barrier_semaphore(), inc=1, device_id={"seq": seq}, device_id_type=MESH
    )


def gather_kernel(
    group, n, u_ref, w_ref, p_ref, u_all, w_all, acc, u_send, u_recv, w_send, up_send, down_send, w_recv, own_sem
):
    me = lax.axis_index("seq")
    outer = me // group
    inner = lax.rem(me, group)
    outers = n // group
    base = outer * group
    length = u_ref.shape[1]
    rows = w_ref.shape[1]
    has_up = outer < outers - 1
    has_down = outer > 0
    barrier = pltpu.get_barrier_semaphore()
    for step in range(1, group):
        greet(base + lax.rem(inner + step, group))

    @pl.when(has_up)
    def _():
        greet(me + group)

    @pl.when(has_down)
    def _():
        greet(me - group)

    pl.semaphore_wait(
        barrier, group - 1 + has_up.astype(jnp.int32) + has_down.astype(jnp.int32)
    )

    def w_slot(source, slot):
        return w_all.at[source, pl.ds(pl.multiple_of(slot * rows, rows), rows), :]

    def u_slot(slot):
        return u_all.at[:, slot]

    own_w = pltpu.make_async_copy(w_ref.at[inner], w_slot(outer, inner), own_sem.at[0])
    own_w.start()
    own_u = pltpu.make_async_copy(u_ref, u_slot(inner), own_sem.at[1])
    own_u.start()

    def up(src, source, slot):
        at = source * group + slot
        return remote(src, w_slot(source, slot), up_send.at[at], w_recv.at[at], me + group)

    def down(src, source, slot):
        at = source * group + slot
        return remote(src, w_slot(source, slot), down_send.at[at], w_recv.at[at], me - group)

    def arrived(source, slot):
        piece = w_slot(source, slot)
        remote(piece, piece, w_send.at[0], w_recv.at[source * group + slot], me).wait_recv()

    sends = []
    for step in range(1, group):
        peer = lax.rem(inner + step, group)
        copy = remote(
            w_ref.at[peer], w_slot(outer, inner), w_send.at[step], w_recv.at[me], base + peer
        )
        copy.start()
        sends.append(copy)

    @pl.when(has_up)
    def _():
        up(w_ref.at[inner], outer, inner).start()

    @pl.when(has_down)
    def _():
        down(w_ref.at[inner], outer, inner).start()

    for step in range(1, group):
        slot = lax.rem(inner + step, group)
        arrived(outer, slot)

        @pl.when(has_up)
        def _():
            up(w_slot(outer, slot), outer, slot).start()

        @pl.when(has_down)
        def _():
            down(w_slot(outer, slot), outer, slot).start()

    for step in range(1, group):
        peer = lax.rem(inner + step, group)
        copy = remote(u_ref, u_slot(inner), u_send.at[step], u_recv.at[inner], base + peer)
        copy.start()
        sends.append(copy)

    def multiply(source, block, first=False):
        part = jnp.dot(u_all[source, block], w_all[source], preferred_element_type=f32)
        if first:
            acc[block] = part
        else:
            acc[block] += part

    def multiply_both(distance, block):
        @pl.when(outer - distance >= 0)
        def _():
            multiply(outer - distance, block)

        @pl.when(outer + distance < outers)
        def _():
            multiply(outer + distance, block)

    def relay(distance, block):
        slot = lax.rem(inner + block, group)

        @pl.when(outer - distance >= 0)
        def _():
            arrived(outer - distance, slot)

            @pl.when(has_up)
            def _():
                up(w_slot(outer - distance, slot), outer - distance, slot).start()

        @pl.when(outer + distance < outers)
        def _():
            arrived(outer + distance, slot)

            @pl.when(has_down)
            def _():
                down(w_slot(outer + distance, slot), outer + distance, slot).start()

    def relay_first(block, carry):
        relay(1, block)
        return carry

    if outers > 1:
        lax.fori_loop(0, group, relay_first, 0)
    own_w.wait()
    own_u.wait()
    for step in range(1, group):
        peer = lax.rem(inner + step, group)
        remote(u_slot(peer), u_slot(peer), u_send.at[0], u_recv.at[peer], me).wait_recv()

    def own_work(block, carry):
        multiply(outer, block, True)
        return carry

    lax.fori_loop(0, group, own_work, 0)

    def later(step, carry):
        distance = step // group
        block = lax.rem(step, group)
        relay(distance, block)
        multiply_both(distance - 1, block)
        return carry

    lax.fori_loop(2 * group, outers * group, later, 0)

    def finish(block, carry):
        if outers > 1:
            multiply_both(outers - 1, block)
        p_ref[block] = acc[block].astype(p_ref.dtype)
        return carry

    lax.fori_loop(0, group, finish, 0)

    def drain(at, carry):
        source = at // group
        slot = lax.rem(at, group)

        @pl.when(jnp.logical_and(has_up, source <= outer))
        def _():
            up(w_slot(source, slot), source, slot).wait_send()

        @pl.when(jnp.logical_and(has_down, source >= outer))
        def _():
            down(w_slot(source, slot), source, slot).wait_send()

        return carry

    lax.fori_loop(0, n, drain, 0)
    for copy in sends:
        copy.wait_send()


def gathered(u, w_parts, n):
    group, rows, columns = w_parts.shape
    outers, length, depth = u.shape
    dma = pltpu.SemaphoreType.DMA
    return pl.pallas_call(
        functools.partial(gather_kernel, group, n),
        out_shape=jax.ShapeDtypeStruct((group, length, columns), bf16),
        in_specs=[pl.BlockSpec(memory_space=pltpu.VMEM)] * 2,
        out_specs=pl.BlockSpec(memory_space=pltpu.VMEM),
        scratch_shapes=[
            pltpu.VMEM((outers, group, length, depth), bf16),
            pltpu.VMEM((outers, group * rows, columns), bf16),
            pltpu.VMEM((group, length, columns), f32),
            dma((group,)),
            dma((group,)),
            dma((group,)),
            dma((n,)),
            dma((n,)),
            dma((n,)),
            dma((2,)),
        ],
        compiler_params=pltpu.CompilerParams(
            collective_id=0, has_side_effects=True, vmem_limit_bytes=56 << 20
        ),
    )(u, w_parts)


def selector(lanes, wide, size, first, stride):
    row = lax.broadcasted_iota(jnp.int32, (lanes, wide), 0)
    head = lax.broadcasted_iota(jnp.int32, (lanes, wide), 1) // size
    return jnp.where(row == head * stride + first, 1.0, 0.0).astype(bf16)


def spread(value, pick):
    high = value.astype(bf16)
    low = (value - high.astype(f32)).astype(bf16)
    return jnp.dot(high, pick, preferred_element_type=f32) + jnp.dot(
        low, pick, preferred_element_type=f32
    )


def silu(value):
    return value / (1.0 + jnp.exp(-value))


def softplus(value):
    return jnp.maximum(value, 0.0) + jnp.log1p(jnp.exp(-jnp.abs(value)))


def state_kernel(
    dims, p_ref, halo_ref, taps_ref, bias_ref, small_bias_ref, rate_ref, x_ref, bc_ref, small_ref, cum_ref, state_ref
):
    wide, state, size, taps = dims
    mixed_ch = wide + 2 * state
    length = p_ref.shape[1]
    raw = p_ref[0, :, :mixed_ch].astype(f32)
    ext = jnp.concatenate([halo_ref[0], raw], axis=0)
    first = halo_ref.shape[1] - taps + 1
    mixed = bias_ref[...] + taps_ref[taps - 1 :] * raw
    for k in range(taps - 1):
        mixed = mixed + taps_ref[k : k + 1] * ext[first + k : first + k + length]
    mixed = silu(mixed)
    x = mixed[:, :wide]
    x_ref[0] = x.astype(bf16)
    bc = mixed[:, wide:].astype(bf16)
    bc_ref[0] = bc
    small = softplus(p_ref[0, :, mixed_ch + wide :].astype(f32) + small_bias_ref[...])
    small_ref[0] = small
    rows = lax.broadcasted_iota(jnp.int32, (length, length), 0)
    cols = lax.broadcasted_iota(jnp.int32, (length, length), 1)
    below = jnp.where(cols <= rows, 1.0, 0.0)
    cum = jnp.dot(
        below,
        -small * rate_ref[...],
        precision=lax.Precision.HIGHEST,
        preferred_element_type=f32,
    )
    cum_ref[0] = cum
    tail = jnp.exp(cum[length - 1 :] - cum) * small
    faded = (x * spread(tail, selector(small.shape[1], wide, size, 0, 1))).astype(bf16)
    state_ref[0] = lax.dot_general(
        bc[:, :state], faded, (((0,), (0,)), ((), ())), preferred_element_type=f32
    )


def inside_kernel(dims, levels, x_ref, bc_ref, small_ref, cum_ref, skip_ref, y_ref):
    wide, state, size, _ = dims
    hs = wide // size
    length = x_ref.shape[1]
    lanes = small_ref.shape[2]
    bc = bc_ref[0]
    scores = lax.dot_general(
        bc[:, state:], bc[:, :state], (((1,), (1,)), ((), ())), preferred_element_type=f32
    )
    rows = lax.broadcasted_iota(jnp.int32, (length, length), 0)
    cols = lax.broadcasted_iota(jnp.int32, (length, length), 1)
    causal = cols <= rows
    small = small_ref[0]
    cum = cum_ref[0]
    cum_rows = jnp.transpose(cum)
    x = x_ref[0].astype(f32)
    stepped = (x * spread(small, selector(lanes, wide, size, 0, 1))).astype(bf16)
    parts = []
    for h in range(hs):
        differ = cum[:, h : h + 1] - cum_rows[h : h + 1, :]
        weights = jnp.exp(jnp.where(causal, differ, -1e30)) * scores
        parts.append(
            jnp.dot(
                weights.astype(bf16),
                stepped[:, h * size : (h + 1) * size],
                preferred_element_type=f32,
            )
        )
    y = jnp.concatenate(parts, axis=1)
    own = spread(small, selector(lanes, wide, size, hs, levels))
    y_ref[0] = y * own + skip_ref[...] * x


def outside_kernel(dims, levels, used, y_ref, bc_ref, bucket_ref, small_ref, cum_ref, p_ref, q_ref):
    wide, state, size, _ = dims
    hs = wide // size
    lanes = small_ref.shape[2]
    c = bc_ref[0, :, state:]
    small = small_ref[0]
    total = None
    for level in range(used):
        reads = jnp.dot(c, bucket_ref[0, level], preferred_element_type=f32)
        term = reads * spread(small, selector(lanes, wide, size, hs + level + 1, levels))
        total = term if total is None else total + term
    y = y_ref[0]
    if total is not None:
        y = y + total * spread(jnp.exp(cum_ref[0]), selector(lanes, wide, size, 0, 1))
    at = wide + 2 * state
    q_ref[0] = (y * silu(p_ref[0, :, at : at + wide].astype(f32))).astype(bf16)


def blocked(shape):
    rest = len(shape) - 1
    return pl.BlockSpec((1,) + tuple(shape[1:]), lambda b: (b,) + (0,) * rest)


def whole(shape):
    rest = len(shape)
    return pl.BlockSpec(tuple(shape), lambda b: (0,) * rest)


def per_block(kernel, group, split, fixed, outs, flops):
    order = split + fixed
    specs = [blocked(v.shape) for v in split] + [whole(v.shape) for v in fixed]
    moved = sum(v.size * v.dtype.itemsize for v in order)
    return pl.pallas_call(
        kernel,
        grid=(group,),
        out_shape=outs,
        in_specs=specs,
        out_specs=[blocked(o.shape) for o in outs],
        compiler_params=pltpu.CompilerParams(vmem_limit_bytes=40 << 20),
        cost_estimate=pl.CostEstimate(flops=flops, bytes_accessed=moved, transcendentals=0),
    )(*order)


def exchange_kernel(group, x_ref, out_ref, send_sem, recv_sem, own_sem):
    me = lax.axis_index("seq")
    inner = lax.rem(me, group)
    base = me - inner
    for step in range(1, group):
        greet(base + lax.rem(inner + step, group))
    pl.semaphore_wait(pltpu.get_barrier_semaphore(), group - 1)
    sends = []
    for step in range(1, group):
        peer = lax.rem(inner + step, group)
        copy = remote(
            x_ref.at[peer], out_ref.at[inner], send_sem.at[step], recv_sem.at[inner], base + peer
        )
        copy.start()
        sends.append(copy)
    own = pltpu.make_async_copy(x_ref.at[inner], out_ref.at[inner], own_sem)
    own.start()
    own.wait()
    for step in range(1, group):
        peer = lax.rem(inner + step, group)
        remote(x_ref.at[peer], out_ref.at[peer], send_sem.at[0], recv_sem.at[peer], me).wait_recv()
    for copy in sends:
        copy.wait_send()


def exchanged(x):
    group = x.shape[0]
    dma = pltpu.SemaphoreType.DMA
    return pl.pallas_call(
        functools.partial(exchange_kernel, group),
        out_shape=jax.ShapeDtypeStruct(x.shape, x.dtype),
        in_specs=[pl.BlockSpec(memory_space=pltpu.VMEM)],
        out_specs=pl.BlockSpec(memory_space=pltpu.VMEM),
        scratch_shapes=[dma((group,)), dma((group,)), dma],
        compiler_params=pltpu.CompilerParams(collective_id=1, has_side_effects=True),
    )(x)


def swapped(block, axis, apart):
    count = lax.axis_size(axis)
    route = []
    for low in range(count):
        high = low | 1 << apart
        if high != low and high < count:
            route += [(low, high), (high, low)]
    return lax.ppermute(block, axis, route)


def from_behind(block, axis, distance):
    devices = range(lax.axis_size(axis))
    route = [(i - distance, i) for i in devices if i - distance in devices]
    return lax.ppermute(block, axis, route)


def passed_along(value, axis, steps):
    count = lax.axis_size(axis)
    pairs = [(source, (source + steps) % count) for source in range(count)]
    return lax.ppermute(value, axis, pairs)


def per_device(
    acts,
    in_proj,
    out_proj,
    conv_weight,
    conv_bias,
    dt_bias,
    decay_rate,
    skip_gain,
    level_bias,
    norm_gain,
    gate_gain,
):
    n = lax.axis_size("seq")
    group = min(4, n)
    bits = group.bit_length() - 1
    position = lax.axis_index("seq")
    inner_at = lax.rem(position, group)
    hidden = acts[0].astype(f32)
    length = hidden.shape[0]
    inner = gate_gain.shape[1]
    heads = dt_bias.shape[1]
    head_size = inner // heads
    chans = conv_weight.shape[2]
    state = (chans - inner) // 2
    taps = conv_weight.shape[1]
    margin = taps - 1
    levels_all = level_bias.shape[1] // heads
    levels_used = n.bit_length() - 1
    wide = inner // group
    hs = heads // group
    tokens = group * length

    w = in_proj[0]
    rows = w.shape[0]

    def cut(lo, count):
        part = w[:, lo : lo + count].reshape(rows, group, count // group)
        return jnp.swapaxes(part, 0, 1)

    shared = jnp.broadcast_to(w[:, inner:chans][None], (group, rows, 2 * state))
    tail = hs + hs * levels_all
    used = 2 * wide + 2 * state + tail
    padded = -(-used // 128) * 128
    w_parts = jnp.concatenate(
        [
            cut(0, inner),
            shared,
            cut(chans, inner),
            cut(chans + inner, heads),
            cut(chans + inner + heads, heads * levels_all),
            jnp.zeros((group, rows, padded - used), w.dtype),
        ],
        axis=2,
    )
    u = (
        hidden * lax.rsqrt(jnp.mean(hidden * hidden, axis=1, keepdims=True) + EPS) * norm_gain[0]
    ).astype(bf16)
    u = jnp.swapaxes(u.reshape(length, n // group, group * rows), 0, 1)
    p = gathered(u, w_parts, n)

    def mine(vector, count):
        return lax.dynamic_slice_in_dim(vector, inner_at * count, count, axis=-1)

    mixed_ch = wide + 2 * state
    dims = (wide, state, head_size, taps)
    lasts = p[:, length - margin :, :mixed_ch]
    earlier = from_behind(lasts[group - 1 :], "seq", group)
    halo = jnp.concatenate([earlier, lasts[: group - 1]], axis=0).astype(f32)
    halo = jnp.pad(halo, ((0, 0), (-margin % 8, 0), (0, 0)))
    taps_w = jnp.concatenate([mine(conv_weight[0][:, :inner], wide), conv_weight[0][:, inner:]], 1)
    taps_b = jnp.concatenate([mine(conv_bias[0][:inner], wide), conv_bias[0][inner:]], 0)[None]
    lanes = padded - mixed_ch - wide
    small_bias = jnp.concatenate([mine(dt_bias[0], hs), mine(level_bias[0], hs * levels_all)])
    small_bias = jnp.pad(small_bias, (0, lanes - tail))[None]
    rate = jnp.pad(mine(decay_rate[0], hs), (0, lanes - hs))[None]
    skip = jnp.repeat(mine(skip_gain[0], hs), head_size)[None]

    def shaped(kind, *sizes):
        return jax.ShapeDtypeStruct((group,) + sizes, kind)

    x, bc, small, cum, states = per_block(
        functools.partial(state_kernel, dims),
        group,
        (p, halo),
        (taps_w, taps_b, small_bias, rate),
        (
            shaped(bf16, length, wide),
            shaped(bf16, length, 2 * state),
            shaped(f32, length, lanes),
            shaped(f32, length, lanes),
            shaped(f32, state, wide),
        ),
        2 * tokens * state * wide,
    )
    (y,) = per_block(
        functools.partial(inside_kernel, dims, levels_all),
        group,
        (x, bc, small, cum),
        (skip,),
        (shaped(f32, length, wide),),
        16 * tokens * length * wide,
    )
    ends = cum[:, length - 1, :hs]

    def faded(log, block):
        return jnp.exp(jnp.repeat(log, head_size))[None] * block

    buckets = [[] for _ in range(group)]
    summed = [states[b] for b in range(group)]
    logs = [ends[b] for b in range(group)]
    before = [jnp.zeros_like(ends[0]) for _ in range(group)]
    for bit in range(bits):
        half = 1 << bit
        merged, merged_logs = [], []
        for g in range(len(summed) // 2):
            low, high = summed[2 * g], summed[2 * g + 1]
            for b in range(2 * g * half, 2 * g * half + half):
                buckets[b].append(jnp.zeros_like(low))
            for b in range(2 * g * half + half, 2 * (g + 1) * half):
                buckets[b].append(faded(before[b], low))
                before[b] = before[b] + logs[2 * g]
            merged.append(faded(logs[2 * g + 1], low) + high)
            merged_logs.append(logs[2 * g] + logs[2 * g + 1])
        summed, logs = merged, merged_logs
    block_state, block_log = summed[0], logs[0]
    before_log = jnp.zeros_like(block_log)
    for bit in range(bits, levels_used):
        other_log, other_state = swapped((block_log, block_state.astype(bf16)), "seq", bit)
        other_state = other_state.astype(f32)
        upper = position >> bit & 1 == 1
        bucket = jnp.where(upper, faded(before_log, other_state), 0.0)
        for b in range(group):
            buckets[b].append(faded(before[b], bucket))
        merged_upper = faded(block_log, other_state) + block_state
        merged_lower = faded(other_log, block_state) + other_state
        block_state = jnp.where(upper, merged_upper, merged_lower)
        before_log = jnp.where(upper, before_log + other_log, before_log)
        block_log = block_log + other_log
    stacked = jnp.stack([jnp.stack(held) for held in buckets]).astype(bf16)
    (gated,) = per_block(
        functools.partial(outside_kernel, dims, levels_all, levels_used),
        group,
        (y, bc, stacked, small, cum, p),
        (),
        (shaped(bf16, length, wide),),
        2 * tokens * state * wide * levels_used,
    )

    own = exchanged(gated)
    own = jnp.swapaxes(own, 0, 1).reshape(length, inner).astype(f32)
    normed = (
        own * lax.rsqrt(jnp.mean(own * own, axis=1, keepdims=True) + EPS) * gate_gain[0]
    ).astype(bf16)
    result = (hidden + jnp.dot(normed, out_proj[0], preferred_element_type=f32)).astype(bf16)
    moved = passed_along(result, "section", 1)
    return moved[None]


def solution(mesh):
    return jax.shard_map(
        per_device,
        mesh=mesh,
        in_specs=(
            P("section", "seq", None),
            P("section", "seq", None),
            P("section", None, None),
            P("section", None, None),
            P("section", None),
            P("section", None),
            P("section", None),
            P("section", None),
            P("section", None),
            P("section", None),
            P("section", None),
        ),
        out_specs=P("section", "seq", None),
        check_vma=False,
    )
```

```python
import functools

import jax
import jax.numpy as jnp
from jax import lax
from jax.experimental import pallas as pl
from jax.experimental.pallas import tpu as pltpu
from jax.sharding import PartitionSpec as P

EPS = 1e-05
MESH = pl.DeviceIdType.MESH
f32 = jnp.float32
bf16 = jnp.bfloat16


def remote(src, dst, send, recv, seq):
    return pltpu.make_async_remote_copy(
        src_ref=src,
        dst_ref=dst,
        send_sem=send,
        recv_sem=recv,
        device_id={"seq": seq},
        device_id_type=MESH,
    )


def greet(seq):
    pl.semaphore_signal(
        pltpu.get_barrier_semaphore(), inc=1, device_id={"seq": seq}, device_id_type=MESH
    )


def gather_kernel(
    group, n, starts, u_ref, w_ref, tail_ref, p_ref, halo_ref,
    u_all, w_all, acc, u_send, u_recv, w_send, up_send, down_send, w_recv,
    bc_up, bc_down, bc_peer, bc_recv, own_sem, halo_sem
):
    me = lax.axis_index("seq")
    outer = me // group
    inner = lax.rem(me, group)
    outers = n // group
    base = outer * group
    length = u_ref.shape[0]
    rows = w_ref.shape[0]
    depth = group * rows
    wide, bc_from, z_from = starts
    lanes = tail_ref.shape[2]
    main = 2 * wide + lanes
    columns = w_all.shape[2]
    has_up = outer < outers - 1
    has_down = outer > 0
    barrier = pltpu.get_barrier_semaphore()
    for step in range(1, group):
        greet(base + lax.rem(inner + step, group))

    @pl.when(has_up)
    def _():
        greet(me + group)

    @pl.when(has_down)
    def _():
        greet(me - group)

    pl.semaphore_wait(
        barrier, group - 1 + has_up.astype(jnp.int32) + has_down.astype(jnp.int32)
    )

    def slot_at(source, slot, lo, hi):
        return w_all.at[source, pl.ds(pl.multiple_of(slot * rows, rows), rows), lo:hi]

    def main_slot(source, slot):
        return slot_at(source, slot, 0, main)

    def bc_slot(source, slot):
        return slot_at(source, slot, main, columns)

    def parts_for(peer):
        at = pl.multiple_of(peer * wide, wide)
        return (
            (w_ref.at[:, pl.ds(at, wide)], 0, wide),
            (w_ref.at[:, pl.ds(pl.multiple_of(z_from + at, 128), wide)], wide, 2 * wide),
            (tail_ref.at[peer], 2 * wide, main),
        )

    bc_src = w_ref.at[:, bc_from : bc_from + columns - main]

    def up(source, slot):
        at = source * group + slot
        piece = main_slot(source, slot)
        return remote(piece, piece, up_send.at[at], w_recv.at[at], me + group)

    def down(source, slot):
        at = source * group + slot
        piece = main_slot(source, slot)
        return remote(piece, piece, down_send.at[at], w_recv.at[at], me - group)

    def along(source, step):
        piece = bc_slot(source, inner)
        here = bc_recv.at[source * group + inner]
        if step > 0:
            return remote(piece, piece, bc_up.at[source], here, me + group)
        return remote(piece, piece, bc_down.at[source], here, me - group)

    def across(source, step):
        piece = bc_slot(source, inner)
        peer = base + lax.rem(inner + step, group)
        at = source * group
        return remote(piece, piece, bc_peer.at[at + step], bc_recv.at[at + inner], peer)

    def arrived(source, slot):
        piece = main_slot(source, slot)
        remote(piece, piece, w_send.at[0], w_recv.at[source * group + slot], me).wait_recv()

    def bc_arrived(source, slot):
        piece = bc_slot(source, slot)
        remote(piece, piece, w_send.at[0], bc_recv.at[source * group + slot], me).wait_recv()

    for src, lo, hi in parts_for(inner):
        pltpu.make_async_copy(src, slot_at(outer, inner, lo, hi), own_sem.at[0]).start()
    pltpu.make_async_copy(bc_src, bc_slot(outer, inner), own_sem.at[0]).start()
    own_u = pltpu.make_async_copy(u_ref, u_all.at[inner], own_sem.at[1])
    own_u.start()
    for step in range(1, group):
        peer = lax.rem(inner + step, group)
        for src, lo, hi in parts_for(peer):
            remote(
                src, slot_at(outer, inner, lo, hi), w_send.at[step], w_recv.at[me], base + peer
            ).start()
    whole_slot = slot_at(outer, inner, 0, columns)
    pltpu.make_async_copy(whole_slot, whole_slot, own_sem.at[0]).wait()

    @pl.when(has_up)
    def _():
        up(outer, inner).start()
        along(outer, 1).start()

    @pl.when(has_down)
    def _():
        down(outer, inner).start()
        along(outer, -1).start()

    for step in range(1, group):
        slot = lax.rem(inner + step, group)
        arrived(outer, slot)

        @pl.when(has_up)
        def _():
            up(outer, slot).start()

        @pl.when(has_down)
        def _():
            down(outer, slot).start()

    sends = []
    for step in range(1, group):
        peer = lax.rem(inner + step, group)
        copy = remote(u_ref, u_all.at[inner], u_send.at[step], u_recv.at[inner], base + peer)
        copy.start()
        sends.append(copy)
        across(outer, step).start()

    chunked = depth % 128 == 0

    def multiply(source, block, first=False):
        if not chunked:
            return

        at = pl.multiple_of(source * depth, 128)
        part = jnp.dot(
            u_all[block, :, pl.ds(at, depth)], w_all[source], preferred_element_type=f32
        )
        if first:
            acc[block] = part
        else:
            acc[block] += part

    def ready(source):
        for step in range(1, group):
            bc_arrived(source, lax.rem(inner + step, group))

    def multiply_both(distance, block):
        @pl.when(outer - distance >= 0)
        def _():
            @pl.when(block == 0)
            def _():
                ready(outer - distance)

            multiply(outer - distance, block)

        @pl.when(outer + distance < outers)
        def _():
            @pl.when(block == 0)
            def _():
                ready(outer + distance)

            multiply(outer + distance, block)

    def relay(distance, block):
        slot = lax.rem(inner + block, group)

        @pl.when(outer - distance >= 0)
        def _():
            source = outer - distance
            arrived(source, slot)

            @pl.when(has_up)
            def _():
                up(source, slot).start()

            @pl.when(block == 0)
            def _():
                bc_arrived(source, inner)

                @pl.when(has_up)
                def _():
                    along(source, 1).start()

                for step in range(1, group):
                    across(source, step).start()

        @pl.when(outer + distance < outers)
        def _():
            source = outer + distance
            arrived(source, slot)

            @pl.when(has_down)
            def _():
                down(source, slot).start()

            @pl.when(block == 0)
            def _():
                bc_arrived(source, inner)

                @pl.when(has_down)
                def _():
                    along(source, -1).start()

                for step in range(1, group):
                    across(source, step).start()

    def relay_first(block, carry):
        relay(1, block)
        return carry

    if outers > 1:
        lax.fori_loop(0, group, relay_first, 0)
    own_u.wait()
    for step in range(1, group):
        peer = lax.rem(inner + step, group)
        remote(u_all.at[peer], u_all.at[peer], u_send.at[0], u_recv.at[peer], me).wait_recv()
    ready(outer)

    def own_work(block, carry):
        multiply(outer, block, True)
        return carry

    lax.fori_loop(0, group, own_work, 0)

    def later(step, carry):
        distance = step // group
        block = lax.rem(step, group)
        relay(distance, block)
        multiply_both(distance - 1, block)
        return carry

    lax.fori_loop(2 * group, outers * group, later, 0)

    def finish(step, carry):
        if outers > 1:
            multiply_both(outers - 1, step)
        if chunked:
            p_ref[step] = acc[step].astype(p_ref.dtype)
        return carry

    lax.fori_loop(0, group, finish, 0)
    if not chunked:
        every = w_all[...].reshape(outers * depth, columns)

        def at_once(block, carry):
            part = jnp.dot(u_all[block], every, preferred_element_type=f32)
            p_ref[block] = part.astype(p_ref.dtype)
            return carry

        lax.fori_loop(0, group, at_once, 0)
    keep = halo_ref.shape[0]

    @pl.when(jnp.logical_not(has_down))
    def _():
        halo_ref[...] = jnp.zeros(halo_ref.shape, halo_ref.dtype)

    def drain(at, carry):
        source = at // group
        slot = lax.rem(at, group)

        @pl.when(jnp.logical_and(has_up, source <= outer))
        def _():
            up(source, slot).wait_send()

            @pl.when(slot == 0)
            def _():
                along(source, 1).wait_send()

        @pl.when(jnp.logical_and(has_down, source >= outer))
        def _():
            down(source, slot).wait_send()

            @pl.when(slot == 0)
            def _():
                along(source, -1).wait_send()

        @pl.when(slot == 0)
        def _():
            for step in range(1, group):
                across(source, step).wait_send()

        return carry

    lax.fori_loop(0, n, drain, 0)
    edge = remote(
        p_ref.at[group - 1, length - keep :], halo_ref, halo_sem.at[0], halo_sem.at[1], me + group
    )

    @pl.when(has_up)
    def _():
        edge.start()

    for copy in sends:
        copy.wait_send()
    for step in range(1, group):
        piece = main_slot(outer, inner)
        remote(piece, piece, w_send.at[step], w_recv.at[me], me).wait_send()

    @pl.when(has_up)
    def _():
        edge.wait_send()

    @pl.when(has_down)
    def _():
        edge.wait_recv()


def gathered(u, w, tails, n, starts):
    group, rows, lanes = tails.shape
    length = u.shape[0]
    outers = n // group
    wide, bc_from, z_from = starts
    columns = 2 * wide + lanes + z_from - bc_from
    dma = pltpu.SemaphoreType.DMA
    return pl.pallas_call(
        functools.partial(gather_kernel, group, n, starts),
        out_shape=(
            jax.ShapeDtypeStruct((group, length, columns), bf16),
            jax.ShapeDtypeStruct((16, columns), bf16),
        ),
        in_specs=[pl.BlockSpec(memory_space=pltpu.VMEM)] * 3,
        out_specs=[pl.BlockSpec(memory_space=pltpu.VMEM)] * 2,
        scratch_shapes=[
            pltpu.VMEM((group,) + u.shape, bf16),
            pltpu.VMEM((outers, group * rows, columns), bf16),
            pltpu.VMEM((group, length, columns), f32),
            dma((group,)),
            dma((group,)),
            dma((group,)),
            dma((n,)),
            dma((n,)),
            dma((n,)),
            dma((outers,)),
            dma((outers,)),
            dma((n,)),
            dma((n,)),
            dma((2,)),
            dma((2,)),
        ],
        compiler_params=pltpu.CompilerParams(
            collective_id=0, has_side_effects=True, vmem_limit_bytes=56 << 20
        ),
    )(u, w, tails)


def selector(lanes, wide, size, first, stride):
    row = lax.broadcasted_iota(jnp.int32, (lanes, wide), 0)
    head = lax.broadcasted_iota(jnp.int32, (lanes, wide), 1) // size
    return jnp.where(row == head * stride + first, 1.0, 0.0).astype(bf16)


def spread(value, pick):
    high = value.astype(bf16)
    low = (value - high.astype(f32)).astype(bf16)
    return jnp.dot(high, pick, preferred_element_type=f32) + jnp.dot(
        low, pick, preferred_element_type=f32
    )


def silu(value):
    return value / (1.0 + jnp.exp(-value))


def softplus(value):
    return jnp.maximum(value, 0.0) + jnp.log1p(jnp.exp(-jnp.abs(value)))


def state_kernel(
    dims, p_ref, before_ref, halo_ref, taps_ref, bias_ref, small_bias_ref, rate_ref, x_ref, bc_ref, small_ref, cum_ref, state_ref
):
    wide, state, size, taps = dims
    length = p_ref.shape[1]
    main = p_ref.shape[2] - 2 * state
    keep = halo_ref.shape[0]
    raw = jnp.concatenate([p_ref[0, :, :wide], p_ref[0, :, main:]], axis=1).astype(f32)
    last = jnp.where(
        pl.program_id(0) == 0, halo_ref[...].astype(f32), before_ref[0].astype(f32)
    )
    last = jnp.concatenate([last[:, :wide], last[:, main:]], axis=1)
    ext = jnp.concatenate([last, raw], axis=0)
    first = keep - taps + 1
    mixed = bias_ref[...] + taps_ref[taps - 1 :] * raw
    for k in range(taps - 1):
        mixed = mixed + taps_ref[k : k + 1] * ext[first + k : first + k + length]
    mixed = silu(mixed)
    x = mixed[:, :wide]
    x_ref[0] = x.astype(bf16)
    bc = mixed[:, wide:].astype(bf16)
    bc_ref[0] = bc
    small = softplus(p_ref[0, :, 2 * wide : main].astype(f32) + small_bias_ref[...])
    small_ref[0] = small
    rows = lax.broadcasted_iota(jnp.int32, (length, length), 0)
    cols = lax.broadcasted_iota(jnp.int32, (length, length), 1)
    below = jnp.where(cols <= rows, 1.0, 0.0)
    cum = jnp.dot(
        below,
        -small * rate_ref[...],
        precision=lax.Precision.HIGHEST,
        preferred_element_type=f32,
    )
    cum_ref[0] = cum
    tail = jnp.exp(cum[length - 1 :] - cum) * small
    faded = (x * spread(tail, selector(small.shape[1], wide, size, 0, 1))).astype(bf16)
    state_ref[0] = lax.dot_general(
        bc[:, :state], faded, (((0,), (0,)), ((), ())), preferred_element_type=f32
    )


def inside_kernel(dims, levels, x_ref, bc_ref, small_ref, cum_ref, skip_ref, y_ref):
    wide, state, size, _ = dims
    hs = wide // size
    length = x_ref.shape[1]
    lanes = small_ref.shape[2]
    bc = bc_ref[0]
    scores = lax.dot_general(
        bc[:, state:], bc[:, :state], (((1,), (1,)), ((), ())), preferred_element_type=f32
    )
    rows = lax.broadcasted_iota(jnp.int32, (length, length), 0)
    cols = lax.broadcasted_iota(jnp.int32, (length, length), 1)
    causal = cols <= rows
    small = small_ref[0]
    cum = cum_ref[0]
    cum_rows = jnp.transpose(cum)
    x = x_ref[0].astype(f32)
    stepped = (x * spread(small, selector(lanes, wide, size, 0, 1))).astype(bf16)
    parts = []
    for h in range(hs):
        differ = cum[:, h : h + 1] - cum_rows[h : h + 1, :]
        weights = jnp.exp(jnp.where(causal, differ, -1e30)) * scores
        parts.append(
            jnp.dot(
                weights.astype(bf16),
                stepped[:, h * size : (h + 1) * size],
                preferred_element_type=f32,
            )
        )
    y = jnp.concatenate(parts, axis=1)
    own = spread(small, selector(lanes, wide, size, hs, levels))
    y_ref[0] = y * own + skip_ref[...] * x


def outside_kernel(
    dims, levels, used, group, y_ref, bc_ref, bucket_ref, small_ref, cum_ref, p_ref, acts_ref, gain_ref, w_hbm,
    out_ref, q_own, q_got, w_ref, acc, w_sem, send_sem, recv_sem
):
    wide, state, size, _ = dims
    hs = wide // size
    lanes = small_ref.shape[2]
    me = lax.axis_index("seq")
    inner = lax.rem(me, group)
    base = me - inner
    load = pltpu.make_async_copy(w_hbm, w_ref, w_sem)
    load.start()
    for step in range(1, group):
        greet(base + lax.rem(inner + step, group))
    pl.semaphore_wait(pltpu.get_barrier_semaphore(), group - 1)

    def copy_to(step):
        peer = lax.rem(inner + step, group)
        return remote(
            q_own.at[peer], q_got.at[inner], send_sem.at[step], recv_sem.at[inner], base + peer
        )

    def work(step, carry):
        block = lax.rem(inner + step, group)
        c = bc_ref[block, :, state:]
        small = small_ref[block]
        total = None
        for level in range(used):
            reads = jnp.dot(c, bucket_ref[block, level], preferred_element_type=f32)
            term = reads * spread(small, selector(lanes, wide, size, hs + level + 1, levels))
            total = term if total is None else total + term
        y = y_ref[block]
        if total is not None:
            y = y + total * spread(jnp.exp(cum_ref[block]), selector(lanes, wide, size, 0, 1))
        z = p_ref[block, :, wide : 2 * wide].astype(f32)
        q_own[block] = (y * silu(z)).astype(bf16)

        @pl.when(step > 1)
        def _():
            copy_to(step - 1).start()

        return carry

    lax.fori_loop(1, group + 1, work, 0)
    load.wait()

    def project(q, j):
        q = q.astype(f32)
        part = jnp.dot(
            (q * gain_ref[j]).astype(bf16), w_ref[j], preferred_element_type=f32
        )
        return part, jnp.sum(q * q, axis=1, keepdims=True)

    acc[...], squares = project(q_own[inner], inner)

    def add(step, squares):
        peer = lax.rem(inner + step, group)
        remote(q_got.at[peer], q_got.at[peer], send_sem.at[0], recv_sem.at[peer], me).wait_recv()
        part, more = project(q_got[peer], peer)
        acc[...] += part
        return squares + more

    squares = lax.fori_loop(1, group, add, squares)
    scale = lax.rsqrt(squares / (wide * group) + EPS)
    out_ref[...] = (acts_ref[...].astype(f32) + acc[...] * scale).astype(bf16)
    for step in range(1, group):
        copy_to(step).wait_send()


def finished(dims, levels, used, args, acts, gains, w):
    group, wide, width = w.shape
    length = acts.shape[0]
    dma = pltpu.SemaphoreType.DMA
    vmem = pl.BlockSpec(memory_space=pltpu.VMEM)
    return pl.pallas_call(
        functools.partial(outside_kernel, dims, levels, used, group),
        out_shape=jax.ShapeDtypeStruct((length, width), bf16),
        in_specs=[vmem] * 8 + [pl.BlockSpec(memory_space=pl.ANY)],
        out_specs=vmem,
        scratch_shapes=[
            pltpu.VMEM((group, length, wide), bf16),
            pltpu.VMEM((group, length, wide), bf16),
            pltpu.VMEM(w.shape, bf16),
            pltpu.VMEM((length, width), f32),
            dma,
            dma((group,)),
            dma((group,)),
        ],
        compiler_params=pltpu.CompilerParams(
            collective_id=1, has_side_effects=True, vmem_limit_bytes=48 << 20
        ),
    )(*args, acts, gains, w)


def blocked(shape):
    rest = len(shape) - 1
    return pl.BlockSpec((1,) + tuple(shape[1:]), lambda b: (b,) + (0,) * rest)


def whole(shape):
    rest = len(shape)
    return pl.BlockSpec(tuple(shape), lambda b: (0,) * rest)


def per_block(kernel, group, split, fixed, outs, flops, edge=0):
    specs = [blocked(v.shape) for v in split]
    if edge:
        p = split[0]
        at = p.shape[1] // edge - 1
        specs.append(
            pl.BlockSpec((1, edge, p.shape[2]), lambda b: (jnp.maximum(b - 1, 0), at, 0))
        )
        split = split + (p,)
    order = split + fixed
    specs += [whole(v.shape) for v in fixed]
    moved = sum(v.size * v.dtype.itemsize for v in order)
    return pl.pallas_call(
        kernel,
        grid=(group,),
        out_shape=outs,
        in_specs=specs,
        out_specs=[blocked(o.shape) for o in outs],
        compiler_params=pltpu.CompilerParams(vmem_limit_bytes=40 << 20),
        cost_estimate=pl.CostEstimate(flops=flops, bytes_accessed=moved, transcendentals=0),
    )(*order)


def exchange_kernel(group, x_ref, out_ref, send_sem, recv_sem, own_sem):
    me = lax.axis_index("seq")
    inner = lax.rem(me, group)
    base = me - inner
    for step in range(1, group):
        greet(base + lax.rem(inner + step, group))
    pl.semaphore_wait(pltpu.get_barrier_semaphore(), group - 1)
    sends = []
    for step in range(1, group):
        peer = lax.rem(inner + step, group)
        copy = remote(
            x_ref.at[peer], out_ref.at[inner], send_sem.at[step], recv_sem.at[inner], base + peer
        )
        copy.start()
        sends.append(copy)
    own = pltpu.make_async_copy(x_ref.at[inner], out_ref.at[inner], own_sem)
    own.start()
    own.wait()
    for step in range(1, group):
        peer = lax.rem(inner + step, group)
        remote(x_ref.at[peer], out_ref.at[peer], send_sem.at[0], recv_sem.at[peer], me).wait_recv()
    for copy in sends:
        copy.wait_send()


def exchanged(x):
    group = x.shape[0]
    dma = pltpu.SemaphoreType.DMA
    return pl.pallas_call(
        functools.partial(exchange_kernel, group),
        out_shape=jax.ShapeDtypeStruct(x.shape, x.dtype),
        in_specs=[pl.BlockSpec(memory_space=pltpu.VMEM)],
        out_specs=pl.BlockSpec(memory_space=pltpu.VMEM),
        scratch_shapes=[dma((group,)), dma((group,)), dma],
        compiler_params=pltpu.CompilerParams(collective_id=1, has_side_effects=True),
    )(x)


def swapped(block, axis, apart):
    count = lax.axis_size(axis)
    route = []
    for low in range(count):
        high = low | 1 << apart
        if high != low and high < count:
            route += [(low, high), (high, low)]
    return lax.ppermute(block, axis, route)


def passed_along(value, axis, steps):
    count = lax.axis_size(axis)
    pairs = [(source, (source + steps) % count) for source in range(count)]
    return lax.ppermute(value, axis, pairs)


def per_device(
    acts,
    in_proj,
    out_proj,
    conv_weight,
    conv_bias,
    dt_bias,
    decay_rate,
    skip_gain,
    level_bias,
    norm_gain,
    gate_gain,
):
    n = lax.axis_size("seq")
    group = min(4, n)
    bits = group.bit_length() - 1
    position = lax.axis_index("seq")
    inner_at = lax.rem(position, group)
    hidden = acts[0].astype(f32)
    length = hidden.shape[0]
    inner = gate_gain.shape[1]
    heads = dt_bias.shape[1]
    head_size = inner // heads
    chans = conv_weight.shape[2]
    state = (chans - inner) // 2
    taps = conv_weight.shape[1]
    margin = taps - 1
    levels_all = level_bias.shape[1] // heads
    levels_used = n.bit_length() - 1
    wide = inner // group
    hs = heads // group
    tokens = group * length

    w = in_proj[0]
    rows = w.shape[0]
    tail = hs + hs * levels_all
    lanes = -(-tail // 128) * 128
    at = chans + inner
    tails = jnp.concatenate(
        [
            w[:, at : at + heads].reshape(rows, group, hs),
            w[:, at + heads :].reshape(rows, group, hs * levels_all),
        ],
        axis=2,
    )
    tails = jnp.swapaxes(jnp.pad(tails, ((0, 0), (0, 0), (0, lanes - tail))), 0, 1)
    u = (
        hidden * lax.rsqrt(jnp.mean(hidden * hidden, axis=1, keepdims=True) + EPS) * norm_gain[0]
    ).astype(bf16)
    p, halo = gathered(u, w, tails, n, (wide, inner, chans))

    def mine(vector, count):
        return lax.dynamic_slice_in_dim(vector, inner_at * count, count, axis=-1)

    dims = (wide, state, head_size, taps)
    taps_w = jnp.concatenate([mine(conv_weight[0][:, :inner], wide), conv_weight[0][:, inner:]], 1)
    taps_b = jnp.concatenate([mine(conv_bias[0][:inner], wide), conv_bias[0][inner:]], 0)[None]
    small_bias = jnp.concatenate([mine(dt_bias[0], hs), mine(level_bias[0], hs * levels_all)])
    small_bias = jnp.pad(small_bias, (0, lanes - tail))[None]
    rate = jnp.pad(mine(decay_rate[0], hs), (0, lanes - hs))[None]
    skip = jnp.repeat(mine(skip_gain[0], hs), head_size)[None]

    def shaped(kind, *sizes):
        return jax.ShapeDtypeStruct((group,) + sizes, kind)

    x, bc, small, cum, states = per_block(
        functools.partial(state_kernel, dims),
        group,
        (p,),
        (halo, taps_w, taps_b, small_bias, rate),
        (
            shaped(bf16, length, wide),
            shaped(bf16, length, 2 * state),
            shaped(f32, length, lanes),
            shaped(f32, length, lanes),
            shaped(f32, state, wide),
        ),
        2 * tokens * state * wide,
        16,
    )
    (y,) = per_block(
        functools.partial(inside_kernel, dims, levels_all),
        group,
        (x, bc, small, cum),
        (skip,),
        (shaped(f32, length, wide),),
        16 * tokens * length * wide,
    )
    ends = cum[:, length - 1, :hs]

    def faded(log, block):
        return jnp.exp(jnp.repeat(log, head_size))[None] * block

    buckets = [[] for _ in range(group)]
    summed = [states[b] for b in range(group)]
    logs = [ends[b] for b in range(group)]
    before = [jnp.zeros_like(ends[0]) for _ in range(group)]
    for bit in range(bits):
        half = 1 << bit
        merged, merged_logs = [], []
        for g in range(len(summed) // 2):
            low, high = summed[2 * g], summed[2 * g + 1]
            for b in range(2 * g * half, 2 * g * half + half):
                buckets[b].append(jnp.zeros_like(low))
            for b in range(2 * g * half + half, 2 * (g + 1) * half):
                buckets[b].append(faded(before[b], low))
                before[b] = before[b] + logs[2 * g]
            merged.append(faded(logs[2 * g + 1], low) + high)
            merged_logs.append(logs[2 * g] + logs[2 * g + 1])
        summed, logs = merged, merged_logs
    block_state, block_log = summed[0], logs[0]
    before_log = jnp.zeros_like(block_log)
    for bit in range(bits, levels_used):
        other_log, other_state = swapped((block_log, block_state.astype(bf16)), "seq", bit)
        other_state = other_state.astype(f32)
        upper = position >> bit & 1 == 1
        bucket = jnp.where(upper, faded(before_log, other_state), 0.0)
        for b in range(group):
            buckets[b].append(faded(before[b], bucket))
        merged_upper = faded(block_log, other_state) + block_state
        merged_lower = faded(other_log, block_state) + other_state
        block_state = jnp.where(upper, merged_upper, merged_lower)
        before_log = jnp.where(upper, before_log + other_log, before_log)
        block_log = block_log + other_log
    stacked = jnp.stack([jnp.stack(held) for held in buckets]).astype(bf16)
    result = finished(
        dims,
        levels_all,
        levels_used,
        (y, bc, stacked, small, cum, p),
        acts[0],
        gate_gain[0].reshape(group, 1, wide),
        out_proj[0].reshape(group, wide, -1),
    )
    moved = passed_along(result, "section", 1)
    return moved[None]


def solution(mesh):
    return jax.shard_map(
        per_device,
        mesh=mesh,
        in_specs=(
            P("section", "seq", None),
            P("section", "seq", None),
            P("section", None, None),
            P("section", None, None),
            P("section", None),
            P("section", None),
            P("section", None),
            P("section", None),
            P("section", None),
            P("section", None),
            P("section", None),
        ),
        out_specs=P("section", "seq", None),
        check_vma=False,
    )
```

```python
import functools

import jax
import jax.numpy as jnp
from jax import lax
from jax.experimental import pallas as pl
from jax.experimental.pallas import tpu as pltpu
from jax.sharding import PartitionSpec as P

EPS = 1e-05
MESH = pl.DeviceIdType.MESH
f32 = jnp.float32
bf16 = jnp.bfloat16


def remote(src, dst, send, recv, seq):
    return pltpu.make_async_remote_copy(
        src_ref=src,
        dst_ref=dst,
        send_sem=send,
        recv_sem=recv,
        device_id={"seq": seq},
        device_id_type=MESH,
    )


def greet(seq):
    pl.semaphore_signal(
        pltpu.get_barrier_semaphore(), inc=1, device_id={"seq": seq}, device_id_type=MESH
    )


def partner(inner, step, group):
    low = lax.rem(lax.rem(inner, 2) + step % 2, 2)
    high = lax.rem(inner // 2 + step // 2, max(group // 2, 1))
    return high * 2 + low


def gather_kernel(
    group, n, starts, u_ref, w_ref, tail_ref, p_ref, halo_ref,
    u_all, w_all, acc, u_send, u_recv, w_send, up_send, down_send, w_recv,
    bc_up, bc_down, bc_peer, bc_recv, own_sem, halo_sem
):
    me = lax.axis_index("seq")
    outer = me // group
    inner = lax.rem(me, group)
    outers = n // group
    base = outer * group
    length = u_ref.shape[0]
    rows = w_ref.shape[0]
    depth = group * rows
    wide, bc_from, z_from = starts
    lanes = tail_ref.shape[2]
    main = 2 * wide + lanes
    columns = w_all.shape[2]
    has_up = outer < outers - 1
    has_down = outer > 0
    barrier = pltpu.get_barrier_semaphore()
    for step in range(1, group):
        greet(base + partner(inner, step, group))

    @pl.when(has_up)
    def _():
        greet(me + group)

    @pl.when(has_down)
    def _():
        greet(me - group)

    pl.semaphore_wait(
        barrier, group - 1 + has_up.astype(jnp.int32) + has_down.astype(jnp.int32)
    )

    def slot_at(source, slot, lo, hi):
        return w_all.at[source, pl.ds(pl.multiple_of(slot * rows, rows), rows), lo:hi]

    def main_slot(source, slot):
        return slot_at(source, slot, 0, main)

    def bc_slot(source, slot):
        return slot_at(source, slot, main, columns)

    def parts_for(peer):
        at = pl.multiple_of(peer * wide, wide)
        return (
            (w_ref.at[:, pl.ds(at, wide)], 0, wide),
            (w_ref.at[:, pl.ds(pl.multiple_of(z_from + at, 128), wide)], wide, 2 * wide),
            (tail_ref.at[peer], 2 * wide, main),
        )

    bc_src = w_ref.at[:, bc_from : bc_from + columns - main]

    def up(source, slot):
        at = source * group + slot
        piece = main_slot(source, slot)
        return remote(piece, piece, up_send.at[at], w_recv.at[at], me + group)

    def down(source, slot):
        at = source * group + slot
        piece = main_slot(source, slot)
        return remote(piece, piece, down_send.at[at], w_recv.at[at], me - group)

    def along(source, step):
        piece = bc_slot(source, inner)
        here = bc_recv.at[source * group + inner]
        if step > 0:
            return remote(piece, piece, bc_up.at[source], here, me + group)
        return remote(piece, piece, bc_down.at[source], here, me - group)

    def across(source, step):
        piece = bc_slot(source, inner)
        peer = base + partner(inner, step, group)
        at = source * group
        return remote(piece, piece, bc_peer.at[at + step], bc_recv.at[at + inner], peer)

    def arrived(source, slot):
        piece = main_slot(source, slot)
        remote(piece, piece, w_send.at[0], w_recv.at[source * group + slot], me).wait_recv()

    def bc_arrived(source, slot):
        piece = bc_slot(source, slot)
        remote(piece, piece, w_send.at[0], bc_recv.at[source * group + slot], me).wait_recv()

    for src, lo, hi in parts_for(inner):
        pltpu.make_async_copy(src, slot_at(outer, inner, lo, hi), own_sem.at[0]).start()
    pltpu.make_async_copy(bc_src, bc_slot(outer, inner), own_sem.at[0]).start()
    own_u = pltpu.make_async_copy(u_ref, u_all.at[inner], own_sem.at[1])
    own_u.start()
    def give(step):
        peer = partner(inner, step, group)
        for src, lo, hi in parts_for(peer):
            remote(
                src, slot_at(outer, inner, lo, hi), w_send.at[step], w_recv.at[me], base + peer
            ).start()

    for step in range(1, min(group, 3)):
        give(step)
    whole_slot = slot_at(outer, inner, 0, columns)
    pltpu.make_async_copy(whole_slot, whole_slot, own_sem.at[0]).wait()

    @pl.when(has_up)
    def _():
        up(outer, inner).start()
        along(outer, 1).start()

    @pl.when(has_down)
    def _():
        down(outer, inner).start()
        along(outer, -1).start()

    for step in range(1, group):
        slot = partner(inner, step, group)
        arrived(outer, slot)
        if step == 1:
            for far in range(3, group):
                give(far)

        @pl.when(has_up)
        def _():
            up(outer, slot).start()

        @pl.when(has_down)
        def _():
            down(outer, slot).start()

    sends = []
    for step in range(1, group):
        peer = partner(inner, step, group)
        copy = remote(u_ref, u_all.at[inner], u_send.at[step], u_recv.at[inner], base + peer)
        copy.start()
        sends.append(copy)
        across(outer, step).start()

    chunked = depth % 128 == 0

    def multiply(source, block, first=False):
        if not chunked:
            return

        at = pl.multiple_of(source * depth, 128)
        part = jnp.dot(
            u_all[block, :, pl.ds(at, depth)], w_all[source], preferred_element_type=f32
        )
        if first:
            acc[block] = part
        else:
            acc[block] += part

    def ready(source):
        for step in range(1, group):
            bc_arrived(source, partner(inner, step, group))

    def multiply_both(distance, block):
        @pl.when(outer - distance >= 0)
        def _():
            @pl.when(block == 0)
            def _():
                ready(outer - distance)

            multiply(outer - distance, block)

        @pl.when(outer + distance < outers)
        def _():
            @pl.when(block == 0)
            def _():
                ready(outer + distance)

            multiply(outer + distance, block)

    def relay(distance, block):
        slot = partner(inner, block, group)

        @pl.when(outer - distance >= 0)
        def _():
            source = outer - distance
            arrived(source, slot)

            @pl.when(has_up)
            def _():
                up(source, slot).start()

            @pl.when(block == 0)
            def _():
                bc_arrived(source, inner)

                @pl.when(has_up)
                def _():
                    along(source, 1).start()

                for step in range(1, group):
                    across(source, step).start()

        @pl.when(outer + distance < outers)
        def _():
            source = outer + distance
            arrived(source, slot)

            @pl.when(has_down)
            def _():
                down(source, slot).start()

            @pl.when(block == 0)
            def _():
                bc_arrived(source, inner)

                @pl.when(has_down)
                def _():
                    along(source, -1).start()

                for step in range(1, group):
                    across(source, step).start()

    def relay_first(block, carry):
        relay(1, block)
        return carry

    def relay_second(block, carry):
        relay(2, block)
        return carry

    if outers > 1:
        lax.fori_loop(0, group, relay_first, 0)
    if outers > 2:
        lax.fori_loop(0, group, relay_second, 0)
    own_u.wait()
    for step in range(1, group):
        peer = partner(inner, step, group)
        remote(u_all.at[peer], u_all.at[peer], u_send.at[0], u_recv.at[peer], me).wait_recv()
    ready(outer)

    def own_work(block, carry):
        multiply(outer, block, True)
        if outers > 2:
            multiply_both(1, block)
        return carry

    lax.fori_loop(0, group, own_work, 0)

    def later(step, carry):
        distance = step // group
        block = lax.rem(step, group)
        relay(distance, block)
        multiply_both(distance - 1, block)
        return carry

    lax.fori_loop(3 * group, max(outers, 3) * group, later, 0)

    def finish(step, carry):
        if outers > 1:
            multiply_both(outers - 1, step)
        if chunked:
            p_ref[step] = acc[step].astype(p_ref.dtype)
        return carry

    lax.fori_loop(0, group, finish, 0)
    if not chunked:
        every = w_all[...].reshape(outers * depth, columns)

        def at_once(block, carry):
            part = jnp.dot(u_all[block], every, preferred_element_type=f32)
            p_ref[block] = part.astype(p_ref.dtype)
            return carry

        lax.fori_loop(0, group, at_once, 0)
    keep = halo_ref.shape[0]

    @pl.when(jnp.logical_not(has_down))
    def _():
        halo_ref[...] = jnp.zeros(halo_ref.shape, halo_ref.dtype)

    def drain(at, carry):
        source = at // group
        slot = lax.rem(at, group)

        @pl.when(jnp.logical_and(has_up, source <= outer))
        def _():
            up(source, slot).wait_send()

            @pl.when(slot == 0)
            def _():
                along(source, 1).wait_send()

        @pl.when(jnp.logical_and(has_down, source >= outer))
        def _():
            down(source, slot).wait_send()

            @pl.when(slot == 0)
            def _():
                along(source, -1).wait_send()

        @pl.when(slot == 0)
        def _():
            for step in range(1, group):
                across(source, step).wait_send()

        return carry

    lax.fori_loop(0, n, drain, 0)
    edge = remote(
        p_ref.at[group - 1, length - keep :], halo_ref, halo_sem.at[0], halo_sem.at[1], me + group
    )

    @pl.when(has_up)
    def _():
        edge.start()

    for copy in sends:
        copy.wait_send()
    for step in range(1, group):
        piece = main_slot(outer, inner)
        remote(piece, piece, w_send.at[step], w_recv.at[me], me).wait_send()

    @pl.when(has_up)
    def _():
        edge.wait_send()

    @pl.when(has_down)
    def _():
        edge.wait_recv()


def gathered(u, w, tails, n, starts):
    group, rows, lanes = tails.shape
    length = u.shape[0]
    outers = n // group
    wide, bc_from, z_from = starts
    columns = 2 * wide + lanes + z_from - bc_from
    dma = pltpu.SemaphoreType.DMA
    return pl.pallas_call(
        functools.partial(gather_kernel, group, n, starts),
        out_shape=(
            jax.ShapeDtypeStruct((group, length, columns), bf16),
            jax.ShapeDtypeStruct((16, columns), bf16),
        ),
        in_specs=[pl.BlockSpec(memory_space=pltpu.VMEM)] * 3,
        out_specs=[pl.BlockSpec(memory_space=pltpu.VMEM)] * 2,
        scratch_shapes=[
            pltpu.VMEM((group,) + u.shape, bf16),
            pltpu.VMEM((outers, group * rows, columns), bf16),
            pltpu.VMEM((group, length, columns), f32),
            dma((group,)),
            dma((group,)),
            dma((group,)),
            dma((n,)),
            dma((n,)),
            dma((n,)),
            dma((outers,)),
            dma((outers,)),
            dma((n,)),
            dma((n,)),
            dma((2,)),
            dma((2,)),
        ],
        compiler_params=pltpu.CompilerParams(
            collective_id=0, has_side_effects=True, vmem_limit_bytes=56 << 20
        ),
    )(u, w, tails)


def selector(lanes, wide, size, first, stride):
    row = lax.broadcasted_iota(jnp.int32, (lanes, wide), 0)
    head = lax.broadcasted_iota(jnp.int32, (lanes, wide), 1) // size
    return jnp.where(row == head * stride + first, 1.0, 0.0).astype(bf16)


def spread(value, pick):
    high = value.astype(bf16)
    low = (value - high.astype(f32)).astype(bf16)
    return jnp.dot(high, pick, preferred_element_type=f32) + jnp.dot(
        low, pick, preferred_element_type=f32
    )


def silu(value):
    return value / (1.0 + jnp.exp(-value))


def softplus(value):
    return jnp.maximum(value, 0.0) + jnp.log1p(jnp.exp(-jnp.abs(value)))


def state_kernel(
    dims, p_ref, before_ref, halo_ref, taps_ref, bias_ref, small_bias_ref, rate_ref, x_ref, bc_ref, small_ref, cum_ref, state_ref
):
    wide, state, size, taps = dims
    length = p_ref.shape[1]
    main = p_ref.shape[2] - 2 * state
    keep = halo_ref.shape[0]
    raw = jnp.concatenate([p_ref[0, :, :wide], p_ref[0, :, main:]], axis=1).astype(f32)
    last = jnp.where(
        pl.program_id(0) == 0, halo_ref[...].astype(f32), before_ref[0].astype(f32)
    )
    last = jnp.concatenate([last[:, :wide], last[:, main:]], axis=1)
    ext = jnp.concatenate([last, raw], axis=0)
    first = keep - taps + 1
    mixed = bias_ref[...] + taps_ref[taps - 1 :] * raw
    for k in range(taps - 1):
        mixed = mixed + taps_ref[k : k + 1] * ext[first + k : first + k + length]
    mixed = silu(mixed)
    x = mixed[:, :wide]
    x_ref[0] = x.astype(bf16)
    bc = mixed[:, wide:].astype(bf16)
    bc_ref[0] = bc
    small = softplus(p_ref[0, :, 2 * wide : main].astype(f32) + small_bias_ref[...])
    small_ref[0] = small
    rows = lax.broadcasted_iota(jnp.int32, (length, length), 0)
    cols = lax.broadcasted_iota(jnp.int32, (length, length), 1)
    below = jnp.where(cols <= rows, 1.0, 0.0)
    cum = jnp.dot(
        below,
        -small * rate_ref[...],
        precision=lax.Precision.HIGHEST,
        preferred_element_type=f32,
    )
    cum_ref[0] = cum
    tail = jnp.exp(cum[length - 1 :] - cum) * small
    faded = (x * spread(tail, selector(small.shape[1], wide, size, 0, 1))).astype(bf16)
    state_ref[0] = lax.dot_general(
        bc[:, :state], faded, (((0,), (0,)), ((), ())), preferred_element_type=f32
    )


def inside_kernel(dims, levels, x_ref, bc_ref, small_ref, cum_ref, skip_ref, y_ref):
    wide, state, size, _ = dims
    hs = wide // size
    length = x_ref.shape[1]
    lanes = small_ref.shape[2]
    bc = bc_ref[0]
    scores = lax.dot_general(
        bc[:, state:], bc[:, :state], (((1,), (1,)), ((), ())), preferred_element_type=f32
    )
    rows = lax.broadcasted_iota(jnp.int32, (length, length), 0)
    cols = lax.broadcasted_iota(jnp.int32, (length, length), 1)
    causal = cols <= rows
    small = small_ref[0]
    cum = cum_ref[0]
    cum_rows = jnp.transpose(cum)
    x = x_ref[0].astype(f32)
    stepped = (x * spread(small, selector(lanes, wide, size, 0, 1))).astype(bf16)
    parts = []
    for h in range(hs):
        differ = cum[:, h : h + 1] - cum_rows[h : h + 1, :]
        weights = jnp.exp(jnp.where(causal, differ, -1e30)) * scores
        parts.append(
            jnp.dot(
                weights.astype(bf16),
                stepped[:, h * size : (h + 1) * size],
                preferred_element_type=f32,
            )
        )
    y = jnp.concatenate(parts, axis=1)
    own = spread(small, selector(lanes, wide, size, hs, levels))
    y_ref[0] = y * own + skip_ref[...] * x


def outside_kernel(
    dims, levels, used, group, y_ref, bc_ref, bucket_ref, small_ref, cum_ref, p_ref, acts_ref, gain_ref, w_hbm,
    out_ref, q_own, q_got, w_ref, acc, w_sem, send_sem, recv_sem
):
    wide, state, size, _ = dims
    hs = wide // size
    lanes = small_ref.shape[2]
    me = lax.axis_index("seq")
    inner = lax.rem(me, group)
    base = me - inner
    load = pltpu.make_async_copy(w_hbm, w_ref, w_sem)
    load.start()
    for step in range(1, group):
        greet(base + partner(inner, group - step, group))
    pl.semaphore_wait(pltpu.get_barrier_semaphore(), group - 1)

    def copy_to(step):
        peer = partner(inner, group - step, group)
        return remote(
            q_own.at[peer], q_got.at[inner], send_sem.at[step], recv_sem.at[inner], base + peer
        )

    def work(step, carry):
        block = partner(inner, group - step, group)
        c = bc_ref[block, :, state:]
        small = small_ref[block]
        total = None
        for level in range(used):
            reads = jnp.dot(c, bucket_ref[block, level], preferred_element_type=f32)
            term = reads * spread(small, selector(lanes, wide, size, hs + level + 1, levels))
            total = term if total is None else total + term
        y = y_ref[block]
        if total is not None:
            y = y + total * spread(jnp.exp(cum_ref[block]), selector(lanes, wide, size, 0, 1))
        z = p_ref[block, :, wide : 2 * wide].astype(f32)
        q_own[block] = (y * silu(z)).astype(bf16)

        @pl.when(step > 1)
        def _():
            copy_to(step - 1).start()

        return carry

    lax.fori_loop(1, group + 1, work, 0)
    load.wait()

    def project(q, j):
        q = q.astype(f32)
        part = jnp.dot(
            (q * gain_ref[j]).astype(bf16), w_ref[j], preferred_element_type=f32
        )
        return part, jnp.sum(q * q, axis=1, keepdims=True)

    acc[...], squares = project(q_own[inner], inner)

    def add(step, squares):
        peer = partner(inner, group - step, group)
        remote(q_got.at[peer], q_got.at[peer], send_sem.at[0], recv_sem.at[peer], me).wait_recv()
        part, more = project(q_got[peer], peer)
        acc[...] += part
        return squares + more

    squares = lax.fori_loop(1, group, add, squares)
    scale = lax.rsqrt(squares / (wide * group) + EPS)
    out_ref[...] = (acts_ref[...].astype(f32) + acc[...] * scale).astype(bf16)
    for step in range(1, group):
        copy_to(step).wait_send()


def finished(dims, levels, used, args, acts, gains, w):
    group, wide, width = w.shape
    length = acts.shape[0]
    dma = pltpu.SemaphoreType.DMA
    vmem = pl.BlockSpec(memory_space=pltpu.VMEM)
    return pl.pallas_call(
        functools.partial(outside_kernel, dims, levels, used, group),
        out_shape=jax.ShapeDtypeStruct((length, width), bf16),
        in_specs=[vmem] * 8 + [pl.BlockSpec(memory_space=pl.ANY)],
        out_specs=vmem,
        scratch_shapes=[
            pltpu.VMEM((group, length, wide), bf16),
            pltpu.VMEM((group, length, wide), bf16),
            pltpu.VMEM(w.shape, bf16),
            pltpu.VMEM((length, width), f32),
            dma,
            dma((group,)),
            dma((group,)),
        ],
        compiler_params=pltpu.CompilerParams(
            collective_id=1, has_side_effects=True, vmem_limit_bytes=48 << 20
        ),
    )(*args, acts, gains, w)


def blocked(shape):
    rest = len(shape) - 1
    return pl.BlockSpec((1,) + tuple(shape[1:]), lambda b: (b,) + (0,) * rest)


def whole(shape):
    rest = len(shape)
    return pl.BlockSpec(tuple(shape), lambda b: (0,) * rest)


def per_block(kernel, group, split, fixed, outs, flops, edge=0):
    specs = [blocked(v.shape) for v in split]
    if edge:
        p = split[0]
        at = p.shape[1] // edge - 1
        specs.append(
            pl.BlockSpec((1, edge, p.shape[2]), lambda b: (jnp.maximum(b - 1, 0), at, 0))
        )
        split = split + (p,)
    order = split + fixed
    specs += [whole(v.shape) for v in fixed]
    moved = sum(v.size * v.dtype.itemsize for v in order)
    return pl.pallas_call(
        kernel,
        grid=(group,),
        out_shape=outs,
        in_specs=specs,
        out_specs=[blocked(o.shape) for o in outs],
        compiler_params=pltpu.CompilerParams(vmem_limit_bytes=40 << 20),
        cost_estimate=pl.CostEstimate(flops=flops, bytes_accessed=moved, transcendentals=0),
    )(*order)


def exchange_kernel(group, x_ref, out_ref, send_sem, recv_sem, own_sem):
    me = lax.axis_index("seq")
    inner = lax.rem(me, group)
    base = me - inner
    for step in range(1, group):
        greet(base + lax.rem(inner + step, group))
    pl.semaphore_wait(pltpu.get_barrier_semaphore(), group - 1)
    sends = []
    for step in range(1, group):
        peer = lax.rem(inner + step, group)
        copy = remote(
            x_ref.at[peer], out_ref.at[inner], send_sem.at[step], recv_sem.at[inner], base + peer
        )
        copy.start()
        sends.append(copy)
    own = pltpu.make_async_copy(x_ref.at[inner], out_ref.at[inner], own_sem)
    own.start()
    own.wait()
    for step in range(1, group):
        peer = lax.rem(inner + step, group)
        remote(x_ref.at[peer], out_ref.at[peer], send_sem.at[0], recv_sem.at[peer], me).wait_recv()
    for copy in sends:
        copy.wait_send()


def exchanged(x):
    group = x.shape[0]
    dma = pltpu.SemaphoreType.DMA
    return pl.pallas_call(
        functools.partial(exchange_kernel, group),
        out_shape=jax.ShapeDtypeStruct(x.shape, x.dtype),
        in_specs=[pl.BlockSpec(memory_space=pltpu.VMEM)],
        out_specs=pl.BlockSpec(memory_space=pltpu.VMEM),
        scratch_shapes=[dma((group,)), dma((group,)), dma],
        compiler_params=pltpu.CompilerParams(collective_id=1, has_side_effects=True),
    )(x)


def swapped(block, axis, apart):
    count = lax.axis_size(axis)
    route = []
    for low in range(count):
        high = low | 1 << apart
        if high != low and high < count:
            route += [(low, high), (high, low)]
    return lax.ppermute(block, axis, route)


def passed_along(value, axis, steps):
    count = lax.axis_size(axis)
    pairs = [(source, (source + steps) % count) for source in range(count)]
    return lax.ppermute(value, axis, pairs)


def per_device(
    acts,
    in_proj,
    out_proj,
    conv_weight,
    conv_bias,
    dt_bias,
    decay_rate,
    skip_gain,
    level_bias,
    norm_gain,
    gate_gain,
):
    n = lax.axis_size("seq")
    group = min(4, n)
    bits = group.bit_length() - 1
    position = lax.axis_index("seq")
    inner_at = lax.rem(position, group)
    hidden = acts[0].astype(f32)
    length = hidden.shape[0]
    inner = gate_gain.shape[1]
    heads = dt_bias.shape[1]
    head_size = inner // heads
    chans = conv_weight.shape[2]
    state = (chans - inner) // 2
    taps = conv_weight.shape[1]
    margin = taps - 1
    levels_all = level_bias.shape[1] // heads
    levels_used = n.bit_length() - 1
    wide = inner // group
    hs = heads // group
    tokens = group * length

    w = in_proj[0]
    rows = w.shape[0]
    tail = hs + hs * levels_all
    lanes = -(-tail // 128) * 128
    at = chans + inner
    tails = jnp.concatenate(
        [
            w[:, at : at + heads].reshape(rows, group, hs),
            w[:, at + heads :].reshape(rows, group, hs * levels_all),
        ],
        axis=2,
    )
    tails = jnp.swapaxes(jnp.pad(tails, ((0, 0), (0, 0), (0, lanes - tail))), 0, 1)
    u = (
        hidden * lax.rsqrt(jnp.mean(hidden * hidden, axis=1, keepdims=True) + EPS) * norm_gain[0]
    ).astype(bf16)
    p, halo = gathered(u, w, tails, n, (wide, inner, chans))

    def mine(vector, count):
        return lax.dynamic_slice_in_dim(vector, inner_at * count, count, axis=-1)

    dims = (wide, state, head_size, taps)
    taps_w = jnp.concatenate([mine(conv_weight[0][:, :inner], wide), conv_weight[0][:, inner:]], 1)
    taps_b = jnp.concatenate([mine(conv_bias[0][:inner], wide), conv_bias[0][inner:]], 0)[None]
    small_bias = jnp.concatenate([mine(dt_bias[0], hs), mine(level_bias[0], hs * levels_all)])
    small_bias = jnp.pad(small_bias, (0, lanes - tail))[None]
    rate = jnp.pad(mine(decay_rate[0], hs), (0, lanes - hs))[None]
    skip = jnp.repeat(mine(skip_gain[0], hs), head_size)[None]

    def shaped(kind, *sizes):
        return jax.ShapeDtypeStruct((group,) + sizes, kind)

    x, bc, small, cum, states = per_block(
        functools.partial(state_kernel, dims),
        group,
        (p,),
        (halo, taps_w, taps_b, small_bias, rate),
        (
            shaped(bf16, length, wide),
            shaped(bf16, length, 2 * state),
            shaped(f32, length, lanes),
            shaped(f32, length, lanes),
            shaped(f32, state, wide),
        ),
        2 * tokens * state * wide,
        16,
    )
    (y,) = per_block(
        functools.partial(inside_kernel, dims, levels_all),
        group,
        (x, bc, small, cum),
        (skip,),
        (shaped(f32, length, wide),),
        16 * tokens * length * wide,
    )
    ends = cum[:, length - 1, :hs]

    def faded(log, block):
        return jnp.exp(jnp.repeat(log, head_size))[None] * block

    buckets = [[] for _ in range(group)]
    summed = [states[b] for b in range(group)]
    logs = [ends[b] for b in range(group)]
    before = [jnp.zeros_like(ends[0]) for _ in range(group)]
    for bit in range(bits):
        half = 1 << bit
        merged, merged_logs = [], []
        for g in range(len(summed) // 2):
            low, high = summed[2 * g], summed[2 * g + 1]
            for b in range(2 * g * half, 2 * g * half + half):
                buckets[b].append(jnp.zeros_like(low))
            for b in range(2 * g * half + half, 2 * (g + 1) * half):
                buckets[b].append(faded(before[b], low))
                before[b] = before[b] + logs[2 * g]
            merged.append(faded(logs[2 * g + 1], low) + high)
            merged_logs.append(logs[2 * g] + logs[2 * g + 1])
        summed, logs = merged, merged_logs
    block_state, block_log = summed[0], logs[0]
    before_log = jnp.zeros_like(block_log)
    for bit in range(bits, levels_used):
        other_log, other_state = swapped((block_log, block_state.astype(bf16)), "seq", bit)
        other_state = other_state.astype(f32)
        upper = position >> bit & 1 == 1
        bucket = jnp.where(upper, faded(before_log, other_state), 0.0)
        for b in range(group):
            buckets[b].append(faded(before[b], bucket))
        merged_upper = faded(block_log, other_state) + block_state
        merged_lower = faded(other_log, block_state) + other_state
        block_state = jnp.where(upper, merged_upper, merged_lower)
        before_log = jnp.where(upper, before_log + other_log, before_log)
        block_log = block_log + other_log
    stacked = jnp.stack([jnp.stack(held) for held in buckets]).astype(bf16)
    result = finished(
        dims,
        levels_all,
        levels_used,
        (y, bc, stacked, small, cum, p),
        acts[0],
        gate_gain[0].reshape(group, 1, wide),
        out_proj[0].reshape(group, wide, -1),
    )
    moved = passed_along(result, "section", 1)
    return moved[None]


def solution(mesh):
    return jax.shard_map(
        per_device,
        mesh=mesh,
        in_specs=(
            P("section", "seq", None),
            P("section", "seq", None),
            P("section", None, None),
            P("section", None, None),
            P("section", None),
            P("section", None),
            P("section", None),
            P("section", None),
            P("section", None),
            P("section", None),
            P("section", None),
        ),
        out_specs=P("section", "seq", None),
        check_vma=False,
    )
```

```python
import functools

import jax
import jax.numpy as jnp
from jax import lax
from jax.experimental import pallas as pl
from jax.experimental.pallas import tpu as pltpu
from jax.sharding import PartitionSpec as P

EPS = 1e-05
MESH = pl.DeviceIdType.MESH
f32 = jnp.float32
bf16 = jnp.bfloat16


def remote(src, dst, send, recv, seq):
    return pltpu.make_async_remote_copy(
        src_ref=src,
        dst_ref=dst,
        send_sem=send,
        recv_sem=recv,
        device_id={"seq": seq},
        device_id_type=MESH,
    )


def greet(seq):
    pl.semaphore_signal(
        pltpu.get_barrier_semaphore(), inc=1, device_id={"seq": seq}, device_id_type=MESH
    )


def partner(inner, step, group):
    low = lax.rem(lax.rem(inner, 2) + step % 2, 2)
    high = lax.rem(inner // 2 + step // 2, max(group // 2, 1))
    return high * 2 + low


def gather_kernel(
    group, n, starts, u_ref, w_ref, tail_ref, p_ref, halo_ref,
    u_all, w_all, acc, u_send, u_recv, w_send, up_send, down_send, w_recv,
    bc_up, bc_down, bc_peer, bc_recv, own_sem, halo_sem
):
    me = lax.axis_index("seq")
    outer = me // group
    inner = lax.rem(me, group)
    outers = n // group
    base = outer * group
    length = u_ref.shape[0]
    rows = w_ref.shape[0]
    depth = group * rows
    wide, bc_from, z_from = starts
    lanes = tail_ref.shape[2]
    main = 2 * wide + lanes
    columns = w_all.shape[2]
    has_up = outer < outers - 1
    has_down = outer > 0
    barrier = pltpu.get_barrier_semaphore()
    for step in range(1, group):
        greet(base + partner(inner, step, group))

    @pl.when(has_up)
    def _():
        greet(me + group)

    @pl.when(has_down)
    def _():
        greet(me - group)

    pl.semaphore_wait(
        barrier, group - 1 + has_up.astype(jnp.int32) + has_down.astype(jnp.int32)
    )

    def slot_at(source, slot, lo, hi):
        return w_all.at[source, pl.ds(pl.multiple_of(slot * rows, rows), rows), lo:hi]

    def main_slot(source, slot):
        return slot_at(source, slot, 0, main)

    def bc_slot(source, slot):
        return slot_at(source, slot, main, columns)

    def parts_for(peer):
        at = pl.multiple_of(peer * wide, wide)
        return (
            (w_ref.at[:, pl.ds(at, wide)], 0, wide),
            (w_ref.at[:, pl.ds(pl.multiple_of(z_from + at, 128), wide)], wide, 2 * wide),
            (tail_ref.at[peer], 2 * wide, main),
        )

    bc_src = w_ref.at[:, bc_from : bc_from + columns - main]

    def up(source, slot):
        at = source * group + slot
        piece = main_slot(source, slot)
        return remote(piece, piece, up_send.at[at], w_recv.at[at], me + group)

    def down(source, slot):
        at = source * group + slot
        piece = main_slot(source, slot)
        return remote(piece, piece, down_send.at[at], w_recv.at[at], me - group)

    def along(source, step):
        piece = bc_slot(source, inner)
        here = bc_recv.at[source * group + inner]
        if step > 0:
            return remote(piece, piece, bc_up.at[source], here, me + group)
        return remote(piece, piece, bc_down.at[source], here, me - group)

    def across(source, step):
        piece = bc_slot(source, inner)
        peer = base + partner(inner, step, group)
        at = source * group
        return remote(piece, piece, bc_peer.at[at + step], bc_recv.at[at + inner], peer)

    def arrived(source, slot):
        piece = main_slot(source, slot)
        remote(piece, piece, w_send.at[0], w_recv.at[source * group + slot], me).wait_recv()

    def bc_arrived(source, slot):
        piece = bc_slot(source, slot)
        remote(piece, piece, w_send.at[0], bc_recv.at[source * group + slot], me).wait_recv()

    for src, lo, hi in parts_for(inner):
        pltpu.make_async_copy(src, slot_at(outer, inner, lo, hi), own_sem.at[0]).start()
    pltpu.make_async_copy(bc_src, bc_slot(outer, inner), own_sem.at[0]).start()
    own_u = pltpu.make_async_copy(u_ref, u_all.at[inner], own_sem.at[1])
    own_u.start()
    def give(step):
        peer = partner(inner, step, group)
        for src, lo, hi in parts_for(peer):
            remote(
                src, slot_at(outer, inner, lo, hi), w_send.at[step], w_recv.at[me], base + peer
            ).start()

    for step in range(1, min(group, 3)):
        give(step)
    whole_slot = slot_at(outer, inner, 0, columns)
    pltpu.make_async_copy(whole_slot, whole_slot, own_sem.at[0]).wait()

    @pl.when(has_up)
    def _():
        up(outer, inner).start()
        along(outer, 1).start()

    @pl.when(has_down)
    def _():
        down(outer, inner).start()
        along(outer, -1).start()

    for step in range(1, group):
        slot = partner(inner, step, group)
        arrived(outer, slot)
        if step == 1:
            for far in range(3, group):
                give(far)

        @pl.when(has_up)
        def _():
            up(outer, slot).start()

        @pl.when(has_down)
        def _():
            down(outer, slot).start()

    sends = []
    for step in range(1, group):
        peer = partner(inner, step, group)
        copy = remote(u_ref, u_all.at[inner], u_send.at[step], u_recv.at[inner], base + peer)
        copy.start()
        sends.append(copy)
        across(outer, step).start()

    chunked = depth % 128 == 0

    def multiply(source, block, first=False):
        if not chunked:
            return

        at = pl.multiple_of(source * depth, 128)
        part = jnp.dot(
            u_all[block, :, pl.ds(at, depth)], w_all[source], preferred_element_type=f32
        )
        if first:
            acc[block] = part
        else:
            acc[block] += part

    def ready(source):
        for step in range(1, group):
            bc_arrived(source, partner(inner, step, group))

    def multiply_both(distance, block):
        @pl.when(outer - distance >= 0)
        def _():
            @pl.when(block == 0)
            def _():
                ready(outer - distance)

            multiply(outer - distance, block)

        @pl.when(outer + distance < outers)
        def _():
            @pl.when(block == 0)
            def _():
                ready(outer + distance)

            multiply(outer + distance, block)

    def relay(distance, block):
        slot = partner(inner, block, group)

        @pl.when(outer - distance >= 0)
        def _():
            source = outer - distance
            arrived(source, slot)

            @pl.when(has_up)
            def _():
                up(source, slot).start()

            @pl.when(block == 0)
            def _():
                bc_arrived(source, inner)

                @pl.when(has_up)
                def _():
                    along(source, 1).start()

                for step in range(1, group):
                    across(source, step).start()

        @pl.when(outer + distance < outers)
        def _():
            source = outer + distance
            arrived(source, slot)

            @pl.when(has_down)
            def _():
                down(source, slot).start()

            @pl.when(block == 0)
            def _():
                bc_arrived(source, inner)

                @pl.when(has_down)
                def _():
                    along(source, -1).start()

                for step in range(1, group):
                    across(source, step).start()

    def relay_first(block, carry):
        relay(1, block)
        return carry

    def relay_second(block, carry):
        relay(2, block)
        return carry

    if outers > 1:
        lax.fori_loop(0, group, relay_first, 0)
    if outers > 2:
        lax.fori_loop(0, group, relay_second, 0)
    own_u.wait()
    for step in range(1, group):
        peer = partner(inner, step, group)
        remote(u_all.at[peer], u_all.at[peer], u_send.at[0], u_recv.at[peer], me).wait_recv()
    ready(outer)

    def own_work(block, carry):
        multiply(outer, block, True)
        if outers > 2:
            multiply_both(1, block)
        return carry

    lax.fori_loop(0, group, own_work, 0)

    def later(step, carry):
        distance = step // group
        block = lax.rem(step, group)
        relay(distance, block)
        multiply_both(distance - 1, block)
        return carry

    lax.fori_loop(3 * group, max(outers, 3) * group, later, 0)

    def finish(step, carry):
        if outers > 1:
            multiply_both(outers - 1, step)
        if chunked:
            p_ref[step] = acc[step].astype(p_ref.dtype)
        return carry

    lax.fori_loop(0, group, finish, 0)
    if not chunked:
        every = w_all[...].reshape(outers * depth, columns)

        def at_once(block, carry):
            part = jnp.dot(u_all[block], every, preferred_element_type=f32)
            p_ref[block] = part.astype(p_ref.dtype)
            return carry

        lax.fori_loop(0, group, at_once, 0)
    keep = halo_ref.shape[0]

    @pl.when(jnp.logical_not(has_down))
    def _():
        halo_ref[...] = jnp.zeros(halo_ref.shape, halo_ref.dtype)

    def drain(at, carry):
        source = at // group
        slot = lax.rem(at, group)

        @pl.when(jnp.logical_and(has_up, source <= outer))
        def _():
            up(source, slot).wait_send()

            @pl.when(slot == 0)
            def _():
                along(source, 1).wait_send()

        @pl.when(jnp.logical_and(has_down, source >= outer))
        def _():
            down(source, slot).wait_send()

            @pl.when(slot == 0)
            def _():
                along(source, -1).wait_send()

        @pl.when(slot == 0)
        def _():
            for step in range(1, group):
                across(source, step).wait_send()

        return carry

    lax.fori_loop(0, n, drain, 0)
    edge = remote(
        p_ref.at[group - 1, length - keep :], halo_ref, halo_sem.at[0], halo_sem.at[1], me + group
    )

    @pl.when(has_up)
    def _():
        edge.start()

    for copy in sends:
        copy.wait_send()
    for step in range(1, group):
        piece = main_slot(outer, inner)
        remote(piece, piece, w_send.at[step], w_recv.at[me], me).wait_send()

    @pl.when(has_up)
    def _():
        edge.wait_send()

    @pl.when(has_down)
    def _():
        edge.wait_recv()


def gathered(u, w, tails, n, starts):
    group, rows, lanes = tails.shape
    length = u.shape[0]
    outers = n // group
    wide, bc_from, z_from = starts
    columns = 2 * wide + lanes + z_from - bc_from
    dma = pltpu.SemaphoreType.DMA
    return pl.pallas_call(
        functools.partial(gather_kernel, group, n, starts),
        out_shape=(
            jax.ShapeDtypeStruct((group, length, columns), bf16),
            jax.ShapeDtypeStruct((16, columns), bf16),
        ),
        in_specs=[pl.BlockSpec(memory_space=pltpu.VMEM)] * 3,
        out_specs=[pl.BlockSpec(memory_space=pltpu.VMEM)] * 2,
        scratch_shapes=[
            pltpu.VMEM((group,) + u.shape, bf16),
            pltpu.VMEM((outers, group * rows, columns), bf16),
            pltpu.VMEM((group, length, columns), f32),
            dma((group,)),
            dma((group,)),
            dma((group,)),
            dma((n,)),
            dma((n,)),
            dma((n,)),
            dma((outers,)),
            dma((outers,)),
            dma((n,)),
            dma((n,)),
            dma((2,)),
            dma((2,)),
        ],
        compiler_params=pltpu.CompilerParams(
            collective_id=0, has_side_effects=True, vmem_limit_bytes=56 << 20
        ),
    )(u, w, tails)


def selector(lanes, wide, size, first, stride):
    row = lax.broadcasted_iota(jnp.int32, (lanes, wide), 0)
    head = lax.broadcasted_iota(jnp.int32, (lanes, wide), 1) // size
    return jnp.where(row == head * stride + first, 1.0, 0.0).astype(bf16)


def spread(value, pick):
    high = value.astype(bf16)
    low = (value - high.astype(f32)).astype(bf16)
    return jnp.dot(high, pick, preferred_element_type=f32) + jnp.dot(
        low, pick, preferred_element_type=f32
    )


def silu(value):
    return value / (1.0 + jnp.exp(-value))


def softplus(value):
    return jnp.maximum(value, 0.0) + jnp.log1p(jnp.exp(-jnp.abs(value)))


def state_kernel(
    dims, p_ref, before_ref, halo_ref, taps_ref, bias_ref, small_bias_ref, rate_ref, x_ref, bc_ref, small_ref, cum_ref, state_ref
):
    wide, state, size, taps = dims
    length = p_ref.shape[1]
    main = p_ref.shape[2] - 2 * state
    keep = halo_ref.shape[0]
    raw = jnp.concatenate([p_ref[0, :, :wide], p_ref[0, :, main:]], axis=1).astype(f32)
    last = jnp.where(
        pl.program_id(0) == 0, halo_ref[...].astype(f32), before_ref[0].astype(f32)
    )
    last = jnp.concatenate([last[:, :wide], last[:, main:]], axis=1)
    ext = jnp.concatenate([last, raw], axis=0)
    first = keep - taps + 1
    mixed = bias_ref[...] + taps_ref[taps - 1 :] * raw
    for k in range(taps - 1):
        mixed = mixed + taps_ref[k : k + 1] * ext[first + k : first + k + length]
    mixed = silu(mixed)
    x = mixed[:, :wide]
    x_ref[0] = x.astype(bf16)
    bc = mixed[:, wide:].astype(bf16)
    bc_ref[0] = bc
    small = softplus(p_ref[0, :, 2 * wide : main].astype(f32) + small_bias_ref[...])
    small_ref[0] = small
    rows = lax.broadcasted_iota(jnp.int32, (length, length), 0)
    cols = lax.broadcasted_iota(jnp.int32, (length, length), 1)
    below = jnp.where(cols <= rows, 1.0, 0.0)
    cum = jnp.dot(
        below,
        -small * rate_ref[...],
        precision=lax.Precision.HIGHEST,
        preferred_element_type=f32,
    )
    cum_ref[0] = cum
    tail = jnp.exp(cum[length - 1 :] - cum) * small
    faded = (x * spread(tail, selector(small.shape[1], wide, size, 0, 1))).astype(bf16)
    state_ref[0] = lax.dot_general(
        bc[:, :state], faded, (((0,), (0,)), ((), ())), preferred_element_type=f32
    )


def inside_kernel(dims, levels, x_ref, bc_ref, small_ref, cum_ref, skip_ref, y_ref):
    wide, state, size, _ = dims
    hs = wide // size
    length = x_ref.shape[1]
    lanes = small_ref.shape[2]
    bc = bc_ref[0]
    scores = lax.dot_general(
        bc[:, state:], bc[:, :state], (((1,), (1,)), ((), ())), preferred_element_type=f32
    )
    rows = lax.broadcasted_iota(jnp.int32, (length, length), 0)
    cols = lax.broadcasted_iota(jnp.int32, (length, length), 1)
    causal = cols <= rows
    small = small_ref[0]
    cum = cum_ref[0]
    cum_rows = jnp.transpose(cum)
    x = x_ref[0].astype(f32)
    stepped = (x * spread(small, selector(lanes, wide, size, 0, 1))).astype(bf16)
    parts = []
    for h in range(hs):
        differ = cum[:, h : h + 1] - cum_rows[h : h + 1, :]
        weights = jnp.exp(jnp.where(causal, differ, -1e30)) * scores
        parts.append(
            jnp.dot(
                weights.astype(bf16),
                stepped[:, h * size : (h + 1) * size],
                preferred_element_type=f32,
            )
        )
    y = jnp.concatenate(parts, axis=1)
    own = spread(small, selector(lanes, wide, size, hs, levels))
    y_ref[0] = y * own + skip_ref[...] * x


def outside_kernel(
    dims, levels, used, group, y_ref, bc_ref, near_ref, far_ref, fade_ref, small_ref, cum_ref, p_ref, acts_ref, gain_ref, w_hbm,
    out_ref, q_own, q_got, w_ref, acc, w_sem, send_sem, recv_sem
):
    wide, state, size, _ = dims
    hs = wide // size
    lanes = small_ref.shape[2]
    me = lax.axis_index("seq")
    inner = lax.rem(me, group)
    base = me - inner
    load = pltpu.make_async_copy(w_hbm, w_ref, w_sem)
    load.start()
    for step in range(1, group):
        greet(base + partner(inner, group - step, group))
    pl.semaphore_wait(pltpu.get_barrier_semaphore(), group - 1)

    def copy_to(step):
        peer = partner(inner, group - step, group)
        return remote(
            q_own.at[peer], q_got.at[inner], send_sem.at[step], recv_sem.at[inner], base + peer
        )

    def work(step, carry):
        block = partner(inner, group - step, group)
        c = bc_ref[block, :, state:]
        small = small_ref[block]
        near = near_ref.shape[1]

        def term(level, bucket):
            reads = jnp.dot(c, bucket, preferred_element_type=f32)
            return reads * spread(small, selector(lanes, wide, size, hs + level + 1, levels))

        total = None
        for level in range(near, used):
            part = term(level, far_ref[level - near])
            total = part if total is None else total + part
        if total is not None:
            total = total * fade_ref[block]
        for level in range(near):
            part = term(level, near_ref[block, level])
            total = part if total is None else total + part
        y = y_ref[block]
        if total is not None:
            y = y + total * spread(jnp.exp(cum_ref[block]), selector(lanes, wide, size, 0, 1))
        z = p_ref[block, :, wide : 2 * wide].astype(f32)
        q_own[block] = (y * silu(z)).astype(bf16)

        @pl.when(step > 1)
        def _():
            copy_to(step - 1).start()

        return carry

    lax.fori_loop(1, group + 1, work, 0)
    load.wait()

    def project(q, j):
        q = q.astype(f32)
        part = jnp.dot(
            (q * gain_ref[j]).astype(bf16), w_ref[j], preferred_element_type=f32
        )
        return part, jnp.sum(q * q, axis=1, keepdims=True)

    acc[...], squares = project(q_own[inner], inner)

    def add(step, squares):
        peer = partner(inner, group - step, group)
        remote(q_got.at[peer], q_got.at[peer], send_sem.at[0], recv_sem.at[peer], me).wait_recv()
        part, more = project(q_got[peer], peer)
        acc[...] += part
        return squares + more

    squares = lax.fori_loop(1, group, add, squares)
    scale = lax.rsqrt(squares / (wide * group) + EPS)
    out_ref[...] = (acts_ref[...].astype(f32) + acc[...] * scale).astype(bf16)
    for step in range(1, group):
        copy_to(step).wait_send()


def finished(dims, levels, used, args, acts, gains, w):
    group, wide, width = w.shape
    length = acts.shape[0]
    dma = pltpu.SemaphoreType.DMA
    vmem = pl.BlockSpec(memory_space=pltpu.VMEM)
    return pl.pallas_call(
        functools.partial(outside_kernel, dims, levels, used, group),
        out_shape=jax.ShapeDtypeStruct((length, width), bf16),
        in_specs=[vmem] * 10 + [pl.BlockSpec(memory_space=pl.ANY)],
        out_specs=vmem,
        scratch_shapes=[
            pltpu.VMEM((group, length, wide), bf16),
            pltpu.VMEM((group, length, wide), bf16),
            pltpu.VMEM(w.shape, bf16),
            pltpu.VMEM((length, width), f32),
            dma,
            dma((group,)),
            dma((group,)),
        ],
        compiler_params=pltpu.CompilerParams(
            collective_id=1, has_side_effects=True, vmem_limit_bytes=48 << 20
        ),
    )(*args, acts, gains, w)


def blocked(shape):
    rest = len(shape) - 1
    return pl.BlockSpec((1,) + tuple(shape[1:]), lambda b: (b,) + (0,) * rest)


def whole(shape):
    rest = len(shape)
    return pl.BlockSpec(tuple(shape), lambda b: (0,) * rest)


def per_block(kernel, group, split, fixed, outs, flops, edge=0):
    specs = [blocked(v.shape) for v in split]
    if edge:
        p = split[0]
        at = p.shape[1] // edge - 1
        specs.append(
            pl.BlockSpec((1, edge, p.shape[2]), lambda b: (jnp.maximum(b - 1, 0), at, 0))
        )
        split = split + (p,)
    order = split + fixed
    specs += [whole(v.shape) for v in fixed]
    moved = sum(v.size * v.dtype.itemsize for v in order)
    return pl.pallas_call(
        kernel,
        grid=(group,),
        out_shape=outs,
        in_specs=specs,
        out_specs=[blocked(o.shape) for o in outs],
        compiler_params=pltpu.CompilerParams(vmem_limit_bytes=40 << 20),
        cost_estimate=pl.CostEstimate(flops=flops, bytes_accessed=moved, transcendentals=0),
    )(*order)


def exchange_kernel(group, x_ref, out_ref, send_sem, recv_sem, own_sem):
    me = lax.axis_index("seq")
    inner = lax.rem(me, group)
    base = me - inner
    for step in range(1, group):
        greet(base + lax.rem(inner + step, group))
    pl.semaphore_wait(pltpu.get_barrier_semaphore(), group - 1)
    sends = []
    for step in range(1, group):
        peer = lax.rem(inner + step, group)
        copy = remote(
            x_ref.at[peer], out_ref.at[inner], send_sem.at[step], recv_sem.at[inner], base + peer
        )
        copy.start()
        sends.append(copy)
    own = pltpu.make_async_copy(x_ref.at[inner], out_ref.at[inner], own_sem)
    own.start()
    own.wait()
    for step in range(1, group):
        peer = lax.rem(inner + step, group)
        remote(x_ref.at[peer], out_ref.at[peer], send_sem.at[0], recv_sem.at[peer], me).wait_recv()
    for copy in sends:
        copy.wait_send()


def exchanged(x):
    group = x.shape[0]
    dma = pltpu.SemaphoreType.DMA
    return pl.pallas_call(
        functools.partial(exchange_kernel, group),
        out_shape=jax.ShapeDtypeStruct(x.shape, x.dtype),
        in_specs=[pl.BlockSpec(memory_space=pltpu.VMEM)],
        out_specs=pl.BlockSpec(memory_space=pltpu.VMEM),
        scratch_shapes=[dma((group,)), dma((group,)), dma],
        compiler_params=pltpu.CompilerParams(collective_id=1, has_side_effects=True),
    )(x)


def swapped(block, axis, apart):
    count = lax.axis_size(axis)
    route = []
    for low in range(count):
        high = low | 1 << apart
        if high != low and high < count:
            route += [(low, high), (high, low)]
    return lax.ppermute(block, axis, route)


def passed_along(value, axis, steps):
    count = lax.axis_size(axis)
    pairs = [(source, (source + steps) % count) for source in range(count)]
    return lax.ppermute(value, axis, pairs)


def per_device(
    acts,
    in_proj,
    out_proj,
    conv_weight,
    conv_bias,
    dt_bias,
    decay_rate,
    skip_gain,
    level_bias,
    norm_gain,
    gate_gain,
):
    n = lax.axis_size("seq")
    group = min(4, n)
    bits = group.bit_length() - 1
    position = lax.axis_index("seq")
    inner_at = lax.rem(position, group)
    hidden = acts[0].astype(f32)
    length = hidden.shape[0]
    inner = gate_gain.shape[1]
    heads = dt_bias.shape[1]
    head_size = inner // heads
    chans = conv_weight.shape[2]
    state = (chans - inner) // 2
    taps = conv_weight.shape[1]
    margin = taps - 1
    levels_all = level_bias.shape[1] // heads
    levels_used = n.bit_length() - 1
    wide = inner // group
    hs = heads // group
    tokens = group * length

    w = in_proj[0]
    rows = w.shape[0]
    tail = hs + hs * levels_all
    lanes = -(-tail // 128) * 128
    at = chans + inner
    tails = jnp.concatenate(
        [
            w[:, at : at + heads].reshape(rows, group, hs),
            w[:, at + heads :].reshape(rows, group, hs * levels_all),
        ],
        axis=2,
    )
    tails = jnp.swapaxes(jnp.pad(tails, ((0, 0), (0, 0), (0, lanes - tail))), 0, 1)
    u = (
        hidden * lax.rsqrt(jnp.mean(hidden * hidden, axis=1, keepdims=True) + EPS) * norm_gain[0]
    ).astype(bf16)
    p, halo = gathered(u, w, tails, n, (wide, inner, chans))

    def mine(vector, count):
        return lax.dynamic_slice_in_dim(vector, inner_at * count, count, axis=-1)

    dims = (wide, state, head_size, taps)
    taps_w = jnp.concatenate([mine(conv_weight[0][:, :inner], wide), conv_weight[0][:, inner:]], 1)
    taps_b = jnp.concatenate([mine(conv_bias[0][:inner], wide), conv_bias[0][inner:]], 0)[None]
    small_bias = jnp.concatenate([mine(dt_bias[0], hs), mine(level_bias[0], hs * levels_all)])
    small_bias = jnp.pad(small_bias, (0, lanes - tail))[None]
    rate = jnp.pad(mine(decay_rate[0], hs), (0, lanes - hs))[None]
    skip = jnp.repeat(mine(skip_gain[0], hs), head_size)[None]

    def shaped(kind, *sizes):
        return jax.ShapeDtypeStruct((group,) + sizes, kind)

    x, bc, small, cum, states = per_block(
        functools.partial(state_kernel, dims),
        group,
        (p,),
        (halo, taps_w, taps_b, small_bias, rate),
        (
            shaped(bf16, length, wide),
            shaped(bf16, length, 2 * state),
            shaped(f32, length, lanes),
            shaped(f32, length, lanes),
            shaped(f32, state, wide),
        ),
        2 * tokens * state * wide,
        16,
    )
    (y,) = per_block(
        functools.partial(inside_kernel, dims, levels_all),
        group,
        (x, bc, small, cum),
        (skip,),
        (shaped(f32, length, wide),),
        16 * tokens * length * wide,
    )
    ends = cum[:, length - 1, :hs]

    def faded(log, block):
        return jnp.exp(jnp.repeat(log, head_size))[None] * block

    buckets = [[] for _ in range(group)]
    summed = [states[b] for b in range(group)]
    logs = [ends[b] for b in range(group)]
    before = [jnp.zeros_like(ends[0]) for _ in range(group)]
    for bit in range(bits):
        half = 1 << bit
        merged, merged_logs = [], []
        for g in range(len(summed) // 2):
            low, high = summed[2 * g], summed[2 * g + 1]
            for b in range(2 * g * half, 2 * g * half + half):
                buckets[b].append(jnp.zeros_like(low))
            for b in range(2 * g * half + half, 2 * (g + 1) * half):
                buckets[b].append(faded(before[b], low))
                before[b] = before[b] + logs[2 * g]
            merged.append(faded(logs[2 * g + 1], low) + high)
            merged_logs.append(logs[2 * g] + logs[2 * g + 1])
        summed, logs = merged, merged_logs
    block_state, block_log = summed[0], logs[0]
    before_log = jnp.zeros_like(block_log)
    far = []
    for bit in range(bits, levels_used):
        other_log, other_state = swapped((block_log, block_state.astype(bf16)), "seq", bit)
        other_state = other_state.astype(f32)
        upper = position >> bit & 1 == 1
        bucket = jnp.where(upper, faded(before_log, other_state), 0.0)
        far.append(bucket.astype(bf16))
        merged_upper = faded(block_log, other_state) + block_state
        merged_lower = faded(other_log, block_state) + other_state
        block_state = jnp.where(upper, merged_upper, merged_lower)
        before_log = jnp.where(upper, before_log + other_log, before_log)
        block_log = block_log + other_log
    near = jnp.stack([jnp.stack(held) for held in buckets]).astype(bf16)
    far = jnp.stack(far)
    fade = jnp.exp(jnp.repeat(jnp.stack(before), head_size, axis=1))[:, None]
    result = finished(
        dims,
        levels_all,
        levels_used,
        (y, bc, near, far, fade, small, cum, p),
        acts[0],
        gate_gain[0].reshape(group, 1, wide),
        out_proj[0].reshape(group, wide, -1),
    )
    moved = passed_along(result, "section", 1)
    return moved[None]


def solution(mesh):
    return jax.shard_map(
        per_device,
        mesh=mesh,
        in_specs=(
            P("section", "seq", None),
            P("section", "seq", None),
            P("section", None, None),
            P("section", None, None),
            P("section", None),
            P("section", None),
            P("section", None),
            P("section", None),
            P("section", None),
            P("section", None),
            P("section", None),
        ),
        out_specs=P("section", "seq", None),
        check_vma=False,
    )
```
